32 devices in a mesh: gx: 4 (over x, core), gy: 8 (over z, y).
Axes of the slice: x: 2, y: 2, z: 4, core: 2. Of those that a mesh axis runs over, the one named last changes fastest.
Arguments:
- populations: float32 [19, 32, 64, 128], P(None, 'gx', 'gy'), may hold values from 0 to 1, as said below
- cell_kind: int32 [32, 64, 128], P('gx', 'gy'), may hold values from 0 to 3, as said below
- outlet_region: int32 [32, 64], P('gx', 'gy'), may hold values from 0 to 63, as said below
Outputs:
- final_populations: float32 [19, 32, 64, 128], P(None, 'gx', 'gy')
- outlet_means: float32 [2, 64], replicated
The draws below stay inside these ranges and needn't reach their ends.
Inputs may be any that keep to these rules, and one draw needn't show every extreme that they name: `populations`: positive. `cell_kind`: the plane z = 0 is all inlet (2), the plane z = 127 all outlet (3); all other cells are fluid (0) or wall (1). `outlet_region`: every region names at least one column; ids are constant on aligned tiles of 4 x 4 columns.
All inputs are finite; a program needn't handle non-finite values.
Results may differ from the reference program's by a relative error of at most 0.0001.
Values sent between devices are 32-bit elements; how exact they have to be, the bound alone decides.
A program may use at most 64 MiB of HBM per device.

```python
import jax
import jax.numpy as jnp
from jax import lax

POPS = 19
REGIONS = 64
STEPS = 2
NX = 32
NY = 64
NZ = 128


DRAW_WEIGHTS = (1.0 / 3.0,) + (1.0 / 18.0,) * 6 + (1.0 / 36.0,) * 12


def draw_populations(key, part):
    place = jnp.arange(NX, dtype=jnp.float32) / NX
    table = jnp.array(DRAW_WEIGHTS, dtype=jnp.float32)
    base = 0.6 + 1.2 * place
    noise = jax.random.uniform(key, (POPS, NX, NY, NZ), jnp.float32, -0.4, 0.4)
    return (table[:, None, None, None] * base[None, :, None, None] * (1.0 + noise)).astype(jnp.float32)


def draw_cell_kind(key, part):
    draws = jax.random.randint(key, (NX, NY, NZ), 0, 100)
    rows_x = jnp.arange(NX, dtype=jnp.int32)
    limit = 10 + 40 * rows_x // NX
    kinds = jnp.where(draws < limit[:, None, None], 1, 0)
    depth = jnp.arange(NZ, dtype=jnp.int32)[None, None, :]
    kinds = jnp.where(depth == 0, 2, kinds)
    kinds = jnp.where(depth == NZ - 1, 3, kinds)
    return kinds.astype(jnp.int32)


def draw_outlet_region(key, part):
    tiles_x = NX // 4
    tiles_y = NY // 4
    chosen = jax.random.permutation(key, tiles_x * tiles_y)[:REGIONS].astype(jnp.int32)
    seed_x = chosen // tiles_y
    seed_y = chosen % tiles_y
    grid_x = jnp.arange(tiles_x, dtype=jnp.int32)[None, :, None]
    grid_y = jnp.arange(tiles_y, dtype=jnp.int32)[None, None, :]
    delta_x = grid_x - seed_x[:, None, None]
    delta_y = grid_y - seed_y[:, None, None]
    distance = delta_x * delta_x + delta_y * delta_y
    tiles = jnp.argmin(distance, axis=0).astype(jnp.int32)
    return jnp.repeat(jnp.repeat(tiles, 4, axis=0), 4, axis=1).astype(jnp.int32)


def setup_inputs(seed: int = 0) -> dict:
    seeds = jax.random.split(jax.random.key(seed), 4)
    populations = draw_populations(jax.random.fold_in(seeds[3], 71), 0)
    cell_kind = draw_cell_kind(jax.random.fold_in(seeds[3], 71), 0)
    outlet_region = draw_outlet_region(jax.random.fold_in(seeds[3], 71), 0)
    return {"populations": populations, "cell_kind": cell_kind, "outlet_region": outlet_region}


VELOCITIES = ((0, 0, 0), (1, 0, 0), (-1, 0, 0), (0, 1, 0), (0, -1, 0), (0, 0, 1), (0, 0, -1), (1, 1, 0), (-1, -1, 0), (1, -1, 0), (-1, 1, 0), (1, 0, 1), (-1, 0, -1), (1, 0, -1), (-1, 0, 1), (0, 1, 1), (0, -1, -1), (0, 1, -1), (0, -1, 1))
WEIGHTS = (1.0 / 3.0,) + (1.0 / 18.0,) * 6 + (1.0 / 36.0,) * 12
OPPOSITE = (0, 2, 1, 4, 3, 6, 5, 8, 7, 10, 9, 12, 11, 14, 13, 16, 15, 18, 17)
RELAX_TIME = 0.8
INLET_SPEED = 0.05


def momentum(current, direction):
    total = jnp.zeros_like(current[0])
    for number in range(19):
        factor = VELOCITIES[number][direction]
        if factor != 0:
            total = total + factor * current[number]
    return total


def equilibrium(density, vel_x, vel_y, vel_z):
    speed_sq = vel_x * vel_x + vel_y * vel_y + vel_z * vel_z
    result = []
    for number in range(19):
        comp_x, comp_y, comp_z = VELOCITIES[number]
        projected = comp_x * vel_x + comp_y * vel_y + comp_z * vel_z
        result.append(WEIGHTS[number] * density * (1.0 + 3.0 * projected + 4.5 * projected * projected - 1.5 * speed_sq))
    return jnp.stack(result)


def collide(current, kinds, col_mean):
    density = jnp.sum(current, axis=0)
    vel_x = momentum(current, 0) / density
    vel_y = momentum(current, 1) / density
    vel_z = momentum(current, 2) / density
    relaxed = current - (current - equilibrium(density, vel_x, vel_y, vel_z)) / RELAX_TIME
    bounced = jnp.stack([current[OPPOSITE[number]] for number in range(19)])
    unity = jnp.ones_like(density)
    still = jnp.zeros_like(density)
    inlet = equilibrium(unity, still, still, INLET_SPEED * unity)
    outlet = equilibrium(col_mean * unity, vel_x, vel_y, vel_z)
    post = jnp.where(kinds == 1, bounced, relaxed)
    post = jnp.where(kinds == 2, inlet, post)
    return jnp.where(kinds == 3, outlet, post)


def stream(post):
    moved = []
    for number in range(19):
        comp_x, comp_y, comp_z = VELOCITIES[number]
        plane = post[number]
        if comp_x == 1:
            plane = jnp.concatenate([jnp.zeros_like(plane[:1]), plane[:-1]], axis=0)
        elif comp_x == -1:
            plane = jnp.concatenate([plane[1:], jnp.zeros_like(plane[:1])], axis=0)
        plane = jnp.roll(plane, comp_y, axis=1)
        plane = jnp.roll(plane, comp_z, axis=2)
        moved.append(plane)
    return jnp.stack(moved)


def reference(populations, cell_kind, outlet_region):
    labels = jnp.arange(REGIONS, dtype=jnp.int32)
    onehot = (outlet_region.reshape(-1)[None, :] == labels[:, None]).astype(jnp.float32)
    is_outlet = cell_kind == 3
    col_count = jnp.sum(is_outlet.astype(jnp.float32), axis=2).reshape(-1)
    counts = jnp.dot(onehot, col_count, precision=lax.Precision.HIGHEST)
    current = populations
    means = []
    for timestep in range(STEPS):
        density = jnp.sum(current, axis=0)
        column = jnp.sum(jnp.where(is_outlet, density, jnp.zeros_like(density)), axis=2).reshape(-1)
        region_mean = jnp.dot(onehot, column, precision=lax.Precision.HIGHEST) / counts
        means.append(region_mean)
        col_mean = jnp.dot(region_mean, onehot, precision=lax.Precision.HIGHEST).reshape(NX, NY)[:, :, None]
        current = stream(collide(current, cell_kind, col_mean))
    return current, jnp.stack(means)
```

```python
import functools

import jax
import jax.numpy as jnp
from jax import lax
from jax.experimental import pallas as pl
from jax.experimental.pallas import tpu as pltpu
from jax.sharding import PartitionSpec as P

REGIONS = 64
TILE = 4
VELOCITIES = (
    (0, 0, 0),
    (1, 0, 0),
    (-1, 0, 0),
    (0, 1, 0),
    (0, -1, 0),
    (0, 0, 1),
    (0, 0, -1),
    (1, 1, 0),
    (-1, -1, 0),
    (1, -1, 0),
    (-1, 1, 0),
    (1, 0, 1),
    (-1, 0, -1),
    (1, 0, -1),
    (-1, 0, 1),
    (0, 1, 1),
    (0, -1, -1),
    (0, 1, -1),
    (0, -1, 1),
)
NUMBER = {velocity: number for number, velocity in enumerate(VELOCITIES)}
WEIGHTS = (1.0 / 3.0,) + (1.0 / 18.0,) * 6 + (1.0 / 36.0,) * 12
OPPOSITE = (0, 2, 1, 4, 3, 6, 5, 8, 7, 10, 9, 12, 11, 14, 13, 16, 15, 18, 17)
RELAX_TIME = 0.8
INLET_SPEED = 0.05
RISING_X = (1, 7, 9, 11, 13)
FALLING_X = (2, 8, 10, 12, 14)
RISING_Y = (3, 7, 10, 15, 17)
FALLING_Y = (4, 8, 9, 16, 18)
SLOTS = RISING_X + FALLING_X + (0, 3, 4, 5, 6, 15, 16, 17, 18)
SLOT = {number: slot for slot, number in enumerate(SLOTS)}
MESH = pl.DeviceIdType.MESH


def inlet_value(number):
    comp_z = VELOCITIES[number][2]
    projected = comp_z * INLET_SPEED
    return WEIGHTS[number] * (
        1.0 + 3.0 * projected + 4.5 * projected * projected - 1.5 * INLET_SPEED * INLET_SPEED
    )


def signed_sum(terms):
    total = None
    for sign, value in terms:
        if total is None:
            total = value if sign > 0 else -value
        else:
            total = total + value if sign > 0 else total - value
    return total


def collide(current, kinds, outlet_density):
    density = functools.reduce(lambda a, b: a + b, current)
    inverse = 1.0 / density
    vel = [
        signed_sum([(v[d], current[n]) for n, v in enumerate(VELOCITIES) if v[d] != 0]) * inverse
        for d in range(3)
    ]
    base = 1.0 - 1.5 * (vel[0] * vel[0] + vel[1] * vel[1] + vel[2] * vel[2])
    wall = kinds == 1
    inlet = kinds == 2
    outlet = kinds == 3
    keep = jnp.where(outlet, 0.0, 1.0 - 1.0 / RELAX_TIME)
    scale = jnp.where(outlet, outlet_density, density * (1.0 / RELAX_TIME))
    scales = {w: scale * w for w in sorted(set(WEIGHTS))}
    post = [None] * 19
    for number in range(19):
        if number > OPPOSITE[number]:
            continue
        other = OPPOSITE[number]
        if number == 0:
            pairs = ((0, base),)
        else:
            projected = signed_sum([(c, vel[d]) for d, c in enumerate(VELOCITIES[number]) if c])
            even = base + 4.5 * projected * projected
            odd = 3.0 * projected
            pairs = ((number, even + odd), (other, even - odd))
        for n, unit in pairs:
            moved = keep * current[n] + scales[WEIGHTS[n]] * unit
            moved = jnp.where(inlet, inlet_value(n), moved)
            post[n] = jnp.where(wall, current[OPPOSITE[n]], moved)
    return density, post


def kernel(
    ngx,
    ngy,
    cx,
    cy,
    region_ref,
    pops_ref,
    kind_ref,
    out_ref,
    means_ref,
    post_a,
    post_b,
    density_ref,
    up_a,
    down_a,
    up_b,
    down_b,
    low_a,
    high_a,
    low_b,
    high_b,
    row_ref,
    table,
    spread,
    mult,
    mult_low,
    mult_high,
    send_sems,
    recv_sems,
    gather_sems,
):
    gx = lax.axis_index("gx")
    gy = lax.axis_index("gy")
    count = ngx * ngy
    me = gx * ngy + gy
    tx_n, ty_n = cx // TILE, cy // TILE
    nz = pops_ref.shape[3]
    lane = lax.broadcasted_iota(jnp.int32, (1, 128), 1)
    zlane = lax.broadcasted_iota(jnp.int32, (cy, nz), 1)
    yrow = lax.broadcasted_iota(jnp.int32, (cy, nz), 0)

    barrier = pltpu.get_barrier_semaphore()

    def greet(k, carry):
        peer = lax.rem(me + k, count)
        pl.semaphore_signal(
            barrier, inc=1, device_id={"gx": peer // ngy, "gy": peer % ngy}, device_id_type=MESH
        )
        return carry

    lax.fori_loop(1, count, greet, 0)

    def first(x, carry):
        current = [pops_ref[n, x] for n in range(19)]
        density, post = collide(current, kind_ref[x], 1.0)
        density_ref[x] = density
        for n in range(19):
            post_a[SLOT[n], x + 1] = post[n]
        for k in range(5):
            up_a[k, x] = post[RISING_Y[k]][cy - 1 :, :]
            down_a[k, x] = post[FALLING_Y[k]][:1, :]
        return carry

    lax.fori_loop(0, cx, first, 0)

    sums = {}

    def put(key, value):
        sums[key] = value if key not in sums else sums[key] + value

    for tx in range(tx_n):
        for i in range(TILE):
            x = tx * TILE + i
            for vx in (-1, 0, 1):
                dx = vx if (vx == 1 and i == TILE - 1) or (vx == -1 and i == 0) else 0
                for vy in (-1, 0, 1):
                    flat = jnp.where(
                        zlane == nz - 1, post_a[SLOT[NUMBER[(vx, vy, 0)]], x + 1], 0.0
                    )
                    if (vx, vy, 1) in NUMBER:
                        rising = post_a[SLOT[NUMBER[(vx, vy, 1)]], x + 1]
                        falling = post_a[SLOT[NUMBER[(vx, vy, -1)]], x + 1]
                        flat = jnp.where(zlane == nz - 2, rising, flat)
                        flat = jnp.where(zlane == 0, falling, flat)
                    put((tx, dx, vy), flat)
            put((tx, "rho"), jnp.where(zlane == nz - 1, density_ref[x], 0.0))
    stage = jnp.zeros((cy, 128), jnp.float32)
    lane8 = lax.broadcasted_iota(jnp.int32, (cy, 128), 1)
    row8 = lax.broadcasted_iota(jnp.int32, (cy, 128), 0)
    block = 16 * ty_n
    for tx in range(tx_n):
        for dx in (-1, 0, 1):
            for vy in (-1, 0, 1):
                value = sums[(tx, dx, vy)]
                fixed = jnp.sum(jnp.where(zlane == nz - 1, 0.0, value), axis=1, keepdims=True)
                scaled = jnp.sum(jnp.where(zlane == nz - 1, value, 0.0), axis=1, keepdims=True)
                at = tx * block + (dx + 1) * 4 + vy + 1
                stage = jnp.where(lane8 == at, fixed, stage)
                stage = jnp.where(lane8 == 64 + at, scaled, stage)
        rho = jnp.sum(sums[(tx, "rho")], axis=1, keepdims=True)
        stage = jnp.where(lane8 == tx * block + 13, rho, stage)
    slot8 = lane8 & 3
    message = jnp.zeros((1, 128), jnp.float32)
    for ty in range(ty_n):
        first_row, last_row = ty * TILE, ty * TILE + TILE - 1
        inside = (row8 >= first_row) & (row8 <= last_row)
        crossing = ((slot8 == 2) & (row8 == last_row)) | ((slot8 == 0) & (row8 == first_row))
        cross = jnp.sum(jnp.where(crossing, stage, 0.0), axis=0, keepdims=True)
        stay = jnp.where(inside & jnp.logical_not(crossing), stage, 0.0)
        stay = jnp.broadcast_to(jnp.sum(stay, axis=0, keepdims=True), (8, 128))
        stay = (stay + pltpu.roll(stay, 1, 1) + pltpu.roll(stay, 127, 1))[:1]
        both = jnp.where((lane & 3) == 1, stay, cross)
        if ty:
            both = pltpu.roll(jnp.broadcast_to(both, (8, 128)), 16 * ty, 1)[:1]
        message = message + both
    for tx in range(tx_n):
        for ty in range(ty_n):
            region = region_ref[tx * TILE, ty * TILE].astype(jnp.float32)
            message = jnp.where(lane == 64 + tx * block + ty * 16 + 13, region, message)
    row_ref[...] = message
    table[me] = message

    pl.semaphore_wait(barrier, count - 1)

    def spread_row(k, carry):
        peer = lax.rem(me + k, count)
        pltpu.make_async_remote_copy(
            src_ref=row_ref,
            dst_ref=table.at[me],
            send_sem=gather_sems.at[0],
            recv_sem=gather_sems.at[1],
            device_id={"gx": peer // ngy, "gy": peer % ngy},
            device_id_type=MESH,
        ).start()
        return carry

    lax.fori_loop(1, count, spread_row, 0)

    def exchange(step, post, up, down, low, high):
        def send(k, source, target, ox, oy):
            copy = pltpu.make_async_remote_copy(
                src_ref=source,
                dst_ref=target,
                send_sem=send_sems.at[step, k],
                recv_sem=recv_sems.at[step, k],
                device_id={"gx": lax.rem(gx + ox + ngx, ngx), "gy": lax.rem(gy + oy + ngy, ngy)},
                device_id_type=MESH,
            )
            copy.start()
            return copy

        return [
            send(0, up.at[RISING_Y.index(7), cx - 1], low.at[RISING_Y.index(7), 0], 1, 1),
            send(1, up.at[RISING_Y.index(10), 0], low.at[RISING_Y.index(10), cx + 1], -1, 1),
            send(2, down.at[FALLING_Y.index(9), cx - 1], high.at[FALLING_Y.index(9), 0], 1, -1),
            send(3, down.at[FALLING_Y.index(8), 0], high.at[FALLING_Y.index(8), cx + 1], -1, -1),
            send(4, up, low.at[:, pl.ds(1, cx)], 0, 1),
            send(5, down, high.at[:, pl.ds(1, cx)], 0, -1),
            send(6, post.at[pl.ds(0, 5), cx], post.at[pl.ds(0, 5), 0], 1, 0),
            send(7, post.at[pl.ds(5, 5), 1], post.at[pl.ds(5, 5), cx + 1], -1, 0),
        ]

    def rims(post, low, high):
        @pl.when(gx == 0)
        def _():
            post[0:5, 0] = jnp.zeros((5, cy, nz), jnp.float32)
            low[RISING_Y.index(7), 0] = jnp.zeros((1, nz), jnp.float32)
            high[FALLING_Y.index(9), 0] = jnp.zeros((1, nz), jnp.float32)

        @pl.when(gx == ngx - 1)
        def _():
            post[5:10, cx + 1] = jnp.zeros((5, cy, nz), jnp.float32)
            low[RISING_Y.index(10), cx + 1] = jnp.zeros((1, nz), jnp.float32)
            high[FALLING_Y.index(8), cx + 1] = jnp.zeros((1, nz), jnp.float32)

    copies = exchange(0, post_a, up_a, down_a, low_a, high_a)

    whole = pltpu.make_async_copy(
        table.at[pl.ds(0, count - 1)], table.at[pl.ds(0, count - 1)], gather_sems.at[1]
    )
    whole.wait()
    pltpu.make_async_copy(
        table.at[pl.ds(0, count - 1)], table.at[pl.ds(0, count - 1)], gather_sems.at[0]
    ).wait()

    tiles = tx_n * ty_n
    lanes = lax.broadcasted_iota(jnp.int32, (ngy, 128), 1)
    lanes_f = lanes.astype(jnp.float32)
    rows = [table[pl.ds(X * ngy, ngy), 0, :] for X in range(ngx)]
    onehot = {}
    total = jnp.zeros((ngy, 128), jnp.float32)
    cells = jnp.zeros((ngy, 128), jnp.float32)
    for X in range(ngx):
        for q in range(tiles):
            at = q * 16 + 13
            onehot[X, q] = rows[X][:, 64 + at : 65 + at] == lanes_f
            total = total + jnp.where(onehot[X, q], rows[X][:, at : at + 1], 0.0)
            cells = cells + jnp.where(onehot[X, q], 1.0 * TILE * TILE, 0.0)
    cells = jnp.sum(cells, axis=0, keepdims=True)
    cells = jnp.where(cells > 0.0, cells, 1.0)
    mean_1 = jnp.sum(total, axis=0, keepdims=True) / cells
    means_ref[0:1, :] = mean_1[:, :REGIONS]

    tile_x, tile_y = (lanes >> 4) // ty_n, (lanes >> 4) % ty_n
    step_x, step_y = ((lanes >> 2) & 3) - 1, (lanes & 3) - 1
    real = (lanes < 16 * tiles) & (step_x < 2) & (step_y < 2)
    to_x, to_y = tile_x + step_x, tile_y + step_y
    off_x = jnp.where(to_x < 0, -1, jnp.where(to_x >= tx_n, 1, 0))
    off_y = jnp.where(to_y < 0, -1, jnp.where(to_y >= ty_n, 1, 0))
    goal = (to_x - off_x * tx_n) * ty_n + (to_y - off_y * ty_n)
    shifted = []
    for X in range(ngx):
        by_tile = jnp.zeros((ngy, 128), jnp.float32)
        for q in range(tiles):
            m = jnp.sum(jnp.where(onehot[X, q], mean_1, 0.0), axis=1, keepdims=True)
            by_tile = jnp.where((lanes >> 4) == q, m, by_tile)
        spread[X] = by_tile
        value = jnp.where(real, rows[X] + by_tile * pltpu.roll(rows[X], 64, 1), 0.0)
        moved = jnp.where(off_y == 0, value, 0.0)
        moved = moved + pltpu.roll(jnp.where(off_y == 1, value, 0.0), 1, 0)
        moved = moved + pltpu.roll(jnp.where(off_y == -1, value, 0.0), ngy - 1, 0)
        shifted.append(moved)
    total = jnp.zeros((ngy, 128), jnp.float32)
    for X in range(ngx):
        landed = jnp.where(off_x == 0, shifted[X], 0.0)
        if X > 0:
            landed = landed + jnp.where(off_x == 1, shifted[X - 1], 0.0)
        if X < ngx - 1:
            landed = landed + jnp.where(off_x == -1, shifted[X + 1], 0.0)
        for q in range(tiles):
            s = jnp.sum(jnp.where(goal == q, landed, 0.0), axis=1, keepdims=True)
            total = total + jnp.where(onehot[X, q], s, 0.0)
    mean_2 = jnp.sum(total, axis=0, keepdims=True) / cells
    means_ref[1:2, :] = mean_2[:, :REGIONS]

    around = {}
    for ox in (-1, 0, 1):
        for oy in (-1, 0, 1):
            sx = jnp.clip(gx + ox, 0, ngx - 1)
            sy = lax.rem(gy + oy + ngy, ngy)
            around[ox, oy] = spread[sx, pl.ds(sy, 1), :]

    def tile_mean(tx, ty):
        ox = -1 if tx < 0 else 1 if tx >= tx_n else 0
        oy = -1 if ty < 0 else 1 if ty >= ty_n else 0
        at = ((tx - ox * tx_n) * ty_n + ty - oy * ty_n) * 16
        return around[ox, oy][:, at : at + 1]

    def columns(values):
        result = values[0]
        for ty in range(1, ty_n):
            result = jnp.where(yrow >= ty * TILE, values[ty], result)
        return result

    zrow = lax.broadcasted_iota(jnp.int32, (1, nz), 1)
    for k in range(tx_n + 2):
        mult[k] = jnp.where(
            zlane == nz - 1, columns([tile_mean(k - 1, ty) for ty in range(ty_n)]), 1.0
        )
        mult_low[k] = jnp.where(zrow == nz - 1, tile_mean(k - 1, -1), 1.0)
        mult_high[k] = jnp.where(zrow == nz - 1, tile_mean(k - 1, ty_n), 1.0)
    outlet_2 = []
    for tx in range(tx_n):
        values = []
        for ty in range(ty_n):
            mine = lane == region_ref[tx * TILE, ty * TILE]
            values.append(jnp.sum(jnp.where(mine, mean_2, 0.0), axis=1, keepdims=True))
        outlet_2.append(columns(values) + jnp.zeros((cy, nz), jnp.float32))

    for copy in copies:
        copy.wait()
    rims(post_a, low_a, high_a)

    def streamed(n, x, post, low, high, scaled):
        vx, vy, vz = VELOCITIES[n]
        source = x + 1 - vx
        block_of = (source + TILE - 1) // TILE
        value = post[SLOT[n], source]
        if scaled:
            value = value * mult[block_of]
        if vy == 1:
            edge = low[RISING_Y.index(n), source]
            edge = edge * mult_low[block_of] if scaled else edge
            value = jnp.where(yrow == 0, edge, pltpu.roll(value, 1, 0))
        elif vy == -1:
            edge = high[FALLING_Y.index(n), source]
            edge = edge * mult_high[block_of] if scaled else edge
            value = jnp.where(yrow == cy - 1, edge, pltpu.roll(value, cy - 1, 0))
        if vz:
            value = pltpu.roll(value, vz % nz, 1)
        return value

    for tx in range(tx_n):

        def second(x, carry):
            current = [streamed(n, x, post_a, low_a, high_a, True) for n in range(19)]
            _, post = collide(current, kind_ref[x], outlet_2[tx])
            for n in range(19):
                post_b[SLOT[n], x + 1] = post[n]
            for k in range(5):
                up_b[k, x] = post[RISING_Y[k]][cy - 1 :, :]
                down_b[k, x] = post[FALLING_Y[k]][:1, :]
            return carry

        lax.fori_loop(tx * TILE, tx * TILE + TILE, second, 0)

    copies = exchange(1, post_b, up_b, down_b, low_b, high_b)
    for copy in copies:
        copy.wait()
    rims(post_b, low_b, high_b)

    def last(x, carry):
        for n in range(19):
            out_ref[n, x] = streamed(n, x, post_b, low_b, high_b, False)
        return carry

    lax.fori_loop(0, cx, last, 0)


def solution(mesh):
    ngx, ngy = mesh.shape["gx"], mesh.shape["gy"]

    def body(populations, cell_kind, outlet_region):
        _, cx, cy, nz = populations.shape
        f32 = jnp.float32
        return pl.pallas_call(
            functools.partial(kernel, ngx, ngy, cx, cy),
            out_shape=(
                jax.ShapeDtypeStruct(populations.shape, f32),
                jax.ShapeDtypeStruct((2, REGIONS), f32),
            ),
            in_specs=[
                pl.BlockSpec(memory_space=pltpu.SMEM),
                pl.BlockSpec(memory_space=pltpu.VMEM),
                pl.BlockSpec(memory_space=pltpu.VMEM),
            ],
            out_specs=(
                pl.BlockSpec(memory_space=pltpu.VMEM),
                pl.BlockSpec(memory_space=pltpu.VMEM),
            ),
            scratch_shapes=[
                pltpu.VMEM((19, cx + 2, cy, nz), f32),
                pltpu.VMEM((19, cx + 2, cy, nz), f32),
                pltpu.VMEM((cx, cy, nz), f32),
                pltpu.VMEM((5, cx, 1, nz), f32),
                pltpu.VMEM((5, cx, 1, nz), f32),
                pltpu.VMEM((5, cx, 1, nz), f32),
                pltpu.VMEM((5, cx, 1, nz), f32),
                pltpu.VMEM((5, cx + 2, 1, nz), f32),
                pltpu.VMEM((5, cx + 2, 1, nz), f32),
                pltpu.VMEM((5, cx + 2, 1, nz), f32),
                pltpu.VMEM((5, cx + 2, 1, nz), f32),
                pltpu.VMEM((1, 128), f32),
                pltpu.VMEM((ngx * ngy, 1, 128), f32),
                pltpu.VMEM((ngx, ngy, 128), f32),
                pltpu.VMEM((cx // TILE + 2, cy, nz), f32),
                pltpu.VMEM((cx // TILE + 2, 1, nz), f32),
                pltpu.VMEM((cx // TILE + 2, 1, nz), f32),
                pltpu.SemaphoreType.DMA((2, 8)),
                pltpu.SemaphoreType.DMA((2, 8)),
                pltpu.SemaphoreType.DMA((2,)),
            ],
            compiler_params=pltpu.CompilerParams(collective_id=0, has_side_effects=True),
        )(outlet_region, populations, cell_kind)

    in_specs = (P(None, "gx", "gy", None), P("gx", "gy", None), P("gx", "gy"))
    out_specs = (P(None, "gx", "gy", None), P())
    return jax.shard_map(body, mesh=mesh, in_specs=in_specs, out_specs=out_specs, check_vma=False)
```

```python
import functools

import jax
import jax.numpy as jnp
from jax import lax
from jax.experimental import pallas as pl
from jax.experimental.pallas import tpu as pltpu
from jax.sharding import PartitionSpec as P

REGIONS = 64
TILE = 4
VELOCITIES = (
    (0, 0, 0),
    (1, 0, 0),
    (-1, 0, 0),
    (0, 1, 0),
    (0, -1, 0),
    (0, 0, 1),
    (0, 0, -1),
    (1, 1, 0),
    (-1, -1, 0),
    (1, -1, 0),
    (-1, 1, 0),
    (1, 0, 1),
    (-1, 0, -1),
    (1, 0, -1),
    (-1, 0, 1),
    (0, 1, 1),
    (0, -1, -1),
    (0, 1, -1),
    (0, -1, 1),
)
NUMBER = {velocity: number for number, velocity in enumerate(VELOCITIES)}
WEIGHTS = (1.0 / 3.0,) + (1.0 / 18.0,) * 6 + (1.0 / 36.0,) * 12
OPPOSITE = (0, 2, 1, 4, 3, 6, 5, 8, 7, 10, 9, 12, 11, 14, 13, 16, 15, 18, 17)
RELAX_TIME = 0.8
INLET_SPEED = 0.05
RISING_X = (1, 7, 9, 11, 13)
FALLING_X = (2, 8, 10, 12, 14)
RISING_Y = (3, 7, 10, 15, 17)
FALLING_Y = (4, 8, 9, 16, 18)
SLOTS = RISING_X + FALLING_X + (0, 3, 4, 5, 6, 15, 16, 17, 18)
SLOT = {number: slot for slot, number in enumerate(SLOTS)}
MESH = pl.DeviceIdType.MESH


def inlet_value(number):
    comp_z = VELOCITIES[number][2]
    projected = comp_z * INLET_SPEED
    return WEIGHTS[number] * (
        1.0 + 3.0 * projected + 4.5 * projected * projected - 1.5 * INLET_SPEED * INLET_SPEED
    )


def signed_sum(terms):
    total = None
    for sign, value in terms:
        if total is None:
            total = value if sign > 0 else -value
        else:
            total = total + value if sign > 0 else total - value
    return total


def collide(current, kinds, outlet_density):
    density = functools.reduce(lambda a, b: a + b, current)
    inverse = 1.0 / density
    vel = [
        signed_sum([(v[d], current[n]) for n, v in enumerate(VELOCITIES) if v[d] != 0]) * inverse
        for d in range(3)
    ]
    base = 1.0 - 1.5 * (vel[0] * vel[0] + vel[1] * vel[1] + vel[2] * vel[2])
    wall = kinds == 1
    inlet = kinds == 2
    outlet = kinds == 3
    keep = jnp.where(outlet, 0.0, 1.0 - 1.0 / RELAX_TIME)
    scale = jnp.where(outlet, outlet_density, density * (1.0 / RELAX_TIME))
    scales = {w: scale * w for w in sorted(set(WEIGHTS))}
    post = [None] * 19
    for number in range(19):
        if number > OPPOSITE[number]:
            continue
        other = OPPOSITE[number]
        if number == 0:
            pairs = ((0, base),)
        else:
            projected = signed_sum([(c, vel[d]) for d, c in enumerate(VELOCITIES[number]) if c])
            even = base + 4.5 * projected * projected
            odd = 3.0 * projected
            pairs = ((number, even + odd), (other, even - odd))
        for n, unit in pairs:
            moved = keep * current[n] + scales[WEIGHTS[n]] * unit
            moved = jnp.where(inlet, inlet_value(n), moved)
            post[n] = jnp.where(wall, current[OPPOSITE[n]], moved)
    return density, post


def streamed(n, x, post, low, high, scales=None):
    vx, vy, vz = VELOCITIES[n]
    source = x + 1 - vx
    cy, nz = post.shape[2:]
    yrow = lax.broadcasted_iota(jnp.int32, (cy, nz), 0)
    value = post[SLOT[n], source]
    if scales:
        scale, scale_low, scale_high = [ref[(source + TILE - 1) // TILE] for ref in scales]
        value = value * scale
    if vy == 1:
        edge = low[RISING_Y.index(n), source]
        edge = edge * scale_low if scales else edge
        value = jnp.where(yrow == 0, edge, pltpu.roll(value, 1, 0))
    elif vy == -1:
        edge = high[FALLING_Y.index(n), source]
        edge = edge * scale_high if scales else edge
        value = jnp.where(yrow == cy - 1, edge, pltpu.roll(value, cy - 1, 0))
    if vz:
        value = pltpu.roll(value, vz % nz, 1)
    return value


def finish(post, low, high, means, out_hbm, means_out, out_ref, sems):
    means_out[...] = means[...]
    copies = []
    for n in range(19):
        for x in range(out_ref.shape[1]):
            out_ref[n, x] = streamed(n, x, post, low, high)
        copies.append(pltpu.make_async_copy(out_ref.at[n], out_hbm.at[n], sems.at[n]))
        copies[-1].start()
    for copy in copies:
        copy.wait()


def kernel(
    ngx,
    ngy,
    cx,
    cy,
    region_ref,
    pops_hbm,
    kind_hbm,
    post_b,
    low_b,
    high_b,
    means_ref,
    pops_ref,
    kind_ref,
    load_sems,
    post_a,
    density_ref,
    up_a,
    down_a,
    up_b,
    down_b,
    low_a,
    high_a,
    row_ref,
    table,
    spread,
    mult,
    mult_low,
    mult_high,
    send_sems,
    recv_sems,
    gather_sems,
):
    gx = lax.axis_index("gx")
    gy = lax.axis_index("gy")
    count = ngx * ngy
    me = gx * ngy + gy
    tx_n, ty_n = cx // TILE, cy // TILE
    nz = pops_ref.shape[3]
    lane = lax.broadcasted_iota(jnp.int32, (1, 128), 1)
    zlane = lax.broadcasted_iota(jnp.int32, (cy, nz), 1)
    yrow = lax.broadcasted_iota(jnp.int32, (cy, nz), 0)

    loads = [
        pltpu.make_async_copy(pops_hbm, pops_ref, load_sems.at[0]),
        pltpu.make_async_copy(kind_hbm, kind_ref, load_sems.at[1]),
    ]
    for load in loads:
        load.start()
    barrier = pltpu.get_barrier_semaphore()

    def wrapped(value, size):
        return jnp.where(value >= size, value - size, value)

    def every_peer(visit):
        for ox in range(ngx):
            px = wrapped(gx + ox, ngx)

            def one(oy, carry):
                visit({"gx": px, "gy": wrapped(gy + oy, ngy)})
                return carry

            lax.fori_loop(0 if ox else 1, ngy, one, 0, unroll=ngy <= 8)

    every_peer(
        lambda peer: pl.semaphore_signal(barrier, inc=1, device_id=peer, device_id_type=MESH)
    )

    def first(x, carry):
        current = [pops_ref[n, x] for n in range(19)]
        density, post = collide(current, kind_ref[x], 1.0)
        density_ref[x] = density
        for n in range(19):
            post_a[SLOT[n], x + 1] = post[n]
        for k in range(5):
            up_a[k, x] = post[RISING_Y[k]][cy - 1 :, :]
            down_a[k, x] = post[FALLING_Y[k]][:1, :]
        return carry

    for load in loads:
        load.wait()
    lax.fori_loop(0, cx, first, 0)

    sums = {}

    def put(key, value):
        sums[key] = value if key not in sums else sums[key] + value

    for tx in range(tx_n):
        for i in range(TILE):
            x = tx * TILE + i
            for vx in (-1, 0, 1):
                dx = vx if (vx == 1 and i == TILE - 1) or (vx == -1 and i == 0) else 0
                for vy in (-1, 0, 1):
                    flat = jnp.where(
                        zlane == nz - 1, post_a[SLOT[NUMBER[(vx, vy, 0)]], x + 1], 0.0
                    )
                    if (vx, vy, 1) in NUMBER:
                        rising = post_a[SLOT[NUMBER[(vx, vy, 1)]], x + 1]
                        falling = post_a[SLOT[NUMBER[(vx, vy, -1)]], x + 1]
                        flat = jnp.where(zlane == nz - 2, rising, flat)
                        flat = jnp.where(zlane == 0, falling, flat)
                    put((tx, dx, vy), flat)
            put((tx, "rho"), jnp.where(zlane == nz - 1, density_ref[x], 0.0))
    stage = jnp.zeros((cy, 128), jnp.float32)
    lane8 = lax.broadcasted_iota(jnp.int32, (cy, 128), 1)
    row8 = lax.broadcasted_iota(jnp.int32, (cy, 128), 0)
    block = 16 * ty_n
    for tx in range(tx_n):
        for dx in (-1, 0, 1):
            for vy in (-1, 0, 1):
                value = sums[(tx, dx, vy)]
                fixed = jnp.sum(jnp.where(zlane == nz - 1, 0.0, value), axis=1, keepdims=True)
                scaled = jnp.sum(jnp.where(zlane == nz - 1, value, 0.0), axis=1, keepdims=True)
                at = tx * block + (dx + 1) * 4 + vy + 1
                stage = jnp.where(lane8 == at, fixed, stage)
                stage = jnp.where(lane8 == 64 + at, scaled, stage)
        rho = jnp.sum(sums[(tx, "rho")], axis=1, keepdims=True)
        stage = jnp.where(lane8 == tx * block + 13, rho, stage)
    slot8 = lane8 & 3
    message = jnp.zeros((1, 128), jnp.float32)
    for ty in range(ty_n):
        first_row, last_row = ty * TILE, ty * TILE + TILE - 1
        inside = (row8 >= first_row) & (row8 <= last_row)
        crossing = ((slot8 == 2) & (row8 == last_row)) | ((slot8 == 0) & (row8 == first_row))
        cross = jnp.sum(jnp.where(crossing, stage, 0.0), axis=0, keepdims=True)
        stay = jnp.where(inside & jnp.logical_not(crossing), stage, 0.0)
        stay = jnp.broadcast_to(jnp.sum(stay, axis=0, keepdims=True), (8, 128))
        stay = (stay + pltpu.roll(stay, 1, 1) + pltpu.roll(stay, 127, 1))[:1]
        both = jnp.where((lane & 3) == 1, stay, cross)
        if ty:
            both = pltpu.roll(jnp.broadcast_to(both, (8, 128)), 16 * ty, 1)[:1]
        message = message + both
    for tx in range(tx_n):
        for ty in range(ty_n):
            region = region_ref[tx * TILE, ty * TILE].astype(jnp.float32)
            message = jnp.where(lane == 64 + tx * block + ty * 16 + 13, region, message)
    row_ref[...] = message
    table[me] = message

    pl.semaphore_wait(barrier, count - 1)

    every_peer(
        lambda peer: pltpu.make_async_remote_copy(
            src_ref=row_ref,
            dst_ref=table.at[me],
            send_sem=gather_sems.at[0],
            recv_sem=gather_sems.at[1],
            device_id=peer,
            device_id_type=MESH,
        ).start()
    )

    def exchange(step, post, up, down, low, high):
        def send(k, source, target, ox, oy):
            copy = pltpu.make_async_remote_copy(
                src_ref=source,
                dst_ref=target,
                send_sem=send_sems.at[step, k],
                recv_sem=recv_sems.at[step, k],
                device_id={"gx": lax.rem(gx + ox + ngx, ngx), "gy": lax.rem(gy + oy + ngy, ngy)},
                device_id_type=MESH,
            )
            copy.start()
            return copy

        return [
            send(0, up.at[RISING_Y.index(7), cx - 1], low.at[RISING_Y.index(7), 0], 1, 1),
            send(1, up.at[RISING_Y.index(10), 0], low.at[RISING_Y.index(10), cx + 1], -1, 1),
            send(2, down.at[FALLING_Y.index(9), cx - 1], high.at[FALLING_Y.index(9), 0], 1, -1),
            send(3, down.at[FALLING_Y.index(8), 0], high.at[FALLING_Y.index(8), cx + 1], -1, -1),
            send(4, up, low.at[:, pl.ds(1, cx)], 0, 1),
            send(5, down, high.at[:, pl.ds(1, cx)], 0, -1),
            send(6, post.at[pl.ds(0, 5), cx], post.at[pl.ds(0, 5), 0], 1, 0),
            send(7, post.at[pl.ds(5, 5), 1], post.at[pl.ds(5, 5), cx + 1], -1, 0),
        ]

    def rims(post, low, high):
        @pl.when(gx == 0)
        def _():
            post[0:5, 0] = jnp.zeros((5, cy, nz), jnp.float32)
            low[RISING_Y.index(7), 0] = jnp.zeros((1, nz), jnp.float32)
            high[FALLING_Y.index(9), 0] = jnp.zeros((1, nz), jnp.float32)

        @pl.when(gx == ngx - 1)
        def _():
            post[5:10, cx + 1] = jnp.zeros((5, cy, nz), jnp.float32)
            low[RISING_Y.index(10), cx + 1] = jnp.zeros((1, nz), jnp.float32)
            high[FALLING_Y.index(8), cx + 1] = jnp.zeros((1, nz), jnp.float32)

    copies = exchange(0, post_a, up_a, down_a, low_a, high_a)

    whole = pltpu.make_async_copy(
        table.at[pl.ds(0, count - 1)], table.at[pl.ds(0, count - 1)], gather_sems.at[1]
    )
    whole.wait()
    pltpu.make_async_copy(
        table.at[pl.ds(0, count - 1)], table.at[pl.ds(0, count - 1)], gather_sems.at[0]
    ).wait()

    tiles = tx_n * ty_n
    lanes = lax.broadcasted_iota(jnp.int32, (ngy, 128), 1)
    lanes_f = lanes.astype(jnp.float32)
    rows = [table[pl.ds(X * ngy, ngy), 0, :] for X in range(ngx)]
    onehot = {}
    total = jnp.zeros((ngy, 128), jnp.float32)
    cells = jnp.zeros((ngy, 128), jnp.float32)
    for X in range(ngx):
        for q in range(tiles):
            at = q * 16 + 13
            onehot[X, q] = rows[X][:, 64 + at : 65 + at] == lanes_f
            total = total + jnp.where(onehot[X, q], rows[X][:, at : at + 1], 0.0)
            cells = cells + jnp.where(onehot[X, q], 1.0 * TILE * TILE, 0.0)
    cells = jnp.sum(cells, axis=0, keepdims=True)
    cells = jnp.where(cells > 0.0, cells, 1.0)
    mean_1 = jnp.sum(total, axis=0, keepdims=True) / cells
    means_ref[0:1, :] = mean_1[:, :REGIONS]

    tile_x, tile_y = (lanes >> 4) // ty_n, (lanes >> 4) % ty_n
    step_x, step_y = ((lanes >> 2) & 3) - 1, (lanes & 3) - 1
    real = (lanes < 16 * tiles) & (step_x < 2) & (step_y < 2)
    to_x, to_y = tile_x + step_x, tile_y + step_y
    off_x = jnp.where(to_x < 0, -1, jnp.where(to_x >= tx_n, 1, 0))
    off_y = jnp.where(to_y < 0, -1, jnp.where(to_y >= ty_n, 1, 0))
    goal = (to_x - off_x * tx_n) * ty_n + (to_y - off_y * ty_n)
    shifted = []
    for X in range(ngx):
        by_tile = jnp.zeros((ngy, 128), jnp.float32)
        for q in range(tiles):
            m = jnp.sum(jnp.where(onehot[X, q], mean_1, 0.0), axis=1, keepdims=True)
            by_tile = jnp.where((lanes >> 4) == q, m, by_tile)
        spread[X] = by_tile
        value = jnp.where(real, rows[X] + by_tile * pltpu.roll(rows[X], 64, 1), 0.0)
        moved = jnp.where(off_y == 0, value, 0.0)
        moved = moved + pltpu.roll(jnp.where(off_y == 1, value, 0.0), 1, 0)
        moved = moved + pltpu.roll(jnp.where(off_y == -1, value, 0.0), ngy - 1, 0)
        shifted.append(moved)
    total = jnp.zeros((ngy, 128), jnp.float32)
    for X in range(ngx):
        landed = jnp.where(off_x == 0, shifted[X], 0.0)
        if X > 0:
            landed = landed + jnp.where(off_x == 1, shifted[X - 1], 0.0)
        if X < ngx - 1:
            landed = landed + jnp.where(off_x == -1, shifted[X + 1], 0.0)
        for q in range(tiles):
            s = jnp.sum(jnp.where(goal == q, landed, 0.0), axis=1, keepdims=True)
            total = total + jnp.where(onehot[X, q], s, 0.0)
    mean_2 = jnp.sum(total, axis=0, keepdims=True) / cells
    means_ref[1:2, :] = mean_2[:, :REGIONS]

    around = {}
    for ox in (-1, 0, 1):
        for oy in (-1, 0, 1):
            sx = jnp.clip(gx + ox, 0, ngx - 1)
            sy = lax.rem(gy + oy + ngy, ngy)
            around[ox, oy] = spread[sx, pl.ds(sy, 1), :]

    def tile_mean(tx, ty):
        ox = -1 if tx < 0 else 1 if tx >= tx_n else 0
        oy = -1 if ty < 0 else 1 if ty >= ty_n else 0
        at = ((tx - ox * tx_n) * ty_n + ty - oy * ty_n) * 16
        return around[ox, oy][:, at : at + 1]

    def columns(values):
        result = values[0]
        for ty in range(1, ty_n):
            result = jnp.where(yrow >= ty * TILE, values[ty], result)
        return result

    zrow = lax.broadcasted_iota(jnp.int32, (1, nz), 1)
    for k in range(tx_n + 2):
        mult[k] = jnp.where(
            zlane == nz - 1, columns([tile_mean(k - 1, ty) for ty in range(ty_n)]), 1.0
        )
        mult_low[k] = jnp.where(zrow == nz - 1, tile_mean(k - 1, -1), 1.0)
        mult_high[k] = jnp.where(zrow == nz - 1, tile_mean(k - 1, ty_n), 1.0)
    outlet_2 = []
    for tx in range(tx_n):
        values = []
        for ty in range(ty_n):
            mine = lane == region_ref[tx * TILE, ty * TILE]
            values.append(jnp.sum(jnp.where(mine, mean_2, 0.0), axis=1, keepdims=True))
        outlet_2.append(columns(values) + jnp.zeros((cy, nz), jnp.float32))

    for copy in copies:
        copy.wait()
    rims(post_a, low_a, high_a)

    for tx in range(tx_n):

        def second(x, carry):
            current = [streamed(n, x, post_a, low_a, high_a, (mult, mult_low, mult_high)) for n in range(19)]
            _, post = collide(current, kind_ref[x], outlet_2[tx])
            for n in range(19):
                post_b[SLOT[n], x + 1] = post[n]
            for k in range(5):
                up_b[k, x] = post[RISING_Y[k]][cy - 1 :, :]
                down_b[k, x] = post[FALLING_Y[k]][:1, :]
            return carry

        lax.fori_loop(tx * TILE, tx * TILE + TILE, second, 0)

    copies = exchange(1, post_b, up_b, down_b, low_b, high_b)
    for copy in copies:
        copy.wait()
    rims(post_b, low_b, high_b)


def solution(mesh):
    ngx, ngy = mesh.shape["gx"], mesh.shape["gy"]

    def body(populations, cell_kind, outlet_region):
        _, cx, cy, nz = populations.shape
        f32 = jnp.float32
        vmem = pl.BlockSpec(memory_space=pltpu.VMEM)
        hbm = pl.BlockSpec(memory_space=pltpu.HBM)
        middle = pl.pallas_call(
            functools.partial(kernel, ngx, ngy, cx, cy),
            out_shape=(
                pltpu.VMEM((19, cx + 2, cy, nz), f32),
                pltpu.VMEM((5, cx + 2, 1, nz), f32),
                pltpu.VMEM((5, cx + 2, 1, nz), f32),
                pltpu.VMEM((2, REGIONS), f32),
            ),
            in_specs=[pl.BlockSpec(memory_space=pltpu.SMEM), hbm, hbm],
            out_specs=(vmem, vmem, vmem, vmem),
            scratch_shapes=[
                pltpu.VMEM(populations.shape, f32),
                pltpu.VMEM(cell_kind.shape, jnp.int32),
                pltpu.SemaphoreType.DMA((2,)),
                pltpu.VMEM((19, cx + 2, cy, nz), f32),
                pltpu.VMEM((cx, cy, nz), f32),
                pltpu.VMEM((5, cx, 1, nz), f32),
                pltpu.VMEM((5, cx, 1, nz), f32),
                pltpu.VMEM((5, cx, 1, nz), f32),
                pltpu.VMEM((5, cx, 1, nz), f32),
                pltpu.VMEM((5, cx + 2, 1, nz), f32),
                pltpu.VMEM((5, cx + 2, 1, nz), f32),
                pltpu.VMEM((1, 128), f32),
                pltpu.VMEM((ngx * ngy, 1, 128), f32),
                pltpu.VMEM((ngx, ngy, 128), f32),
                pltpu.VMEM((cx // TILE + 2, cy, nz), f32),
                pltpu.VMEM((cx // TILE + 2, 1, nz), f32),
                pltpu.VMEM((cx // TILE + 2, 1, nz), f32),
                pltpu.SemaphoreType.DMA((2, 8)),
                pltpu.SemaphoreType.DMA((2, 8)),
                pltpu.SemaphoreType.DMA((2,)),
            ],
            compiler_params=pltpu.CompilerParams(
                collective_id=0, has_side_effects=True, vmem_limit_bytes=48 * 2**20
            ),
        )(outlet_region, populations, cell_kind)
        return pl.pallas_call(
            finish,
            out_shape=(
                jax.ShapeDtypeStruct(populations.shape, f32),
                jax.ShapeDtypeStruct((2, REGIONS), f32),
            ),
            in_specs=[vmem, vmem, vmem, vmem],
            out_specs=(hbm, vmem),
            scratch_shapes=[
                pltpu.VMEM(populations.shape, f32),
                pltpu.SemaphoreType.DMA((19,)),
            ],
            compiler_params=pltpu.CompilerParams(vmem_limit_bytes=16 * 2**20),
        )(*middle)

    in_specs = (P(None, "gx", "gy", None), P("gx", "gy", None), P("gx", "gy"))
    out_specs = (P(None, "gx", "gy", None), P())
    return jax.shard_map(body, mesh=mesh, in_specs=in_specs, out_specs=out_specs, check_vma=False)
```

```python
import functools

import jax
import jax.numpy as jnp
from jax import lax
from jax.experimental import pallas as pl
from jax.experimental.pallas import tpu as pltpu
from jax.sharding import PartitionSpec as P

REGIONS = 64
TILE = 4
VELOCITIES = (
    (0, 0, 0),
    (1, 0, 0),
    (-1, 0, 0),
    (0, 1, 0),
    (0, -1, 0),
    (0, 0, 1),
    (0, 0, -1),
    (1, 1, 0),
    (-1, -1, 0),
    (1, -1, 0),
    (-1, 1, 0),
    (1, 0, 1),
    (-1, 0, -1),
    (1, 0, -1),
    (-1, 0, 1),
    (0, 1, 1),
    (0, -1, -1),
    (0, 1, -1),
    (0, -1, 1),
)
NUMBER = {velocity: number for number, velocity in enumerate(VELOCITIES)}
WEIGHTS = (1.0 / 3.0,) + (1.0 / 18.0,) * 6 + (1.0 / 36.0,) * 12
OPPOSITE = (0, 2, 1, 4, 3, 6, 5, 8, 7, 10, 9, 12, 11, 14, 13, 16, 15, 18, 17)
RELAX_TIME = 0.8
INLET_SPEED = 0.05
RISING_X = (1, 7, 9, 11, 13)
FALLING_X = (2, 8, 10, 12, 14)
RISING_Y = (3, 7, 10, 15, 17)
FALLING_Y = (4, 8, 9, 16, 18)
SLOTS = RISING_X + FALLING_X + (0, 3, 4, 5, 6, 15, 16, 17, 18)
SLOT = {number: slot for slot, number in enumerate(SLOTS)}
MESH = pl.DeviceIdType.MESH


def inlet_value(number):
    comp_z = VELOCITIES[number][2]
    projected = comp_z * INLET_SPEED
    return WEIGHTS[number] * (
        1.0 + 3.0 * projected + 4.5 * projected * projected - 1.5 * INLET_SPEED * INLET_SPEED
    )


def signed_sum(terms):
    total = None
    for sign, value in terms:
        if total is None:
            total = value if sign > 0 else -value
        else:
            total = total + value if sign > 0 else total - value
    return total


def collide(current, kinds, outlet_density):
    density = functools.reduce(lambda a, b: a + b, current)
    inverse = 1.0 / density
    vel = [
        signed_sum([(v[d], current[n]) for n, v in enumerate(VELOCITIES) if v[d] != 0]) * inverse
        for d in range(3)
    ]
    base = 1.0 - 1.5 * (vel[0] * vel[0] + vel[1] * vel[1] + vel[2] * vel[2])
    wall = kinds == 1
    inlet = kinds == 2
    outlet = kinds == 3
    keep = jnp.where(outlet, 0.0, 1.0 - 1.0 / RELAX_TIME)
    scale = jnp.where(outlet, outlet_density, density * (1.0 / RELAX_TIME))
    scales = {w: scale * w for w in sorted(set(WEIGHTS))}
    post = [None] * 19
    for number in range(19):
        if number > OPPOSITE[number]:
            continue
        other = OPPOSITE[number]
        if number == 0:
            pairs = ((0, base),)
        else:
            projected = signed_sum([(c, vel[d]) for d, c in enumerate(VELOCITIES[number]) if c])
            even = base + 4.5 * projected * projected
            odd = 3.0 * projected
            pairs = ((number, even + odd), (other, even - odd))
        for n, unit in pairs:
            moved = keep * current[n] + scales[WEIGHTS[n]] * unit
            moved = jnp.where(inlet, inlet_value(n), moved)
            post[n] = jnp.where(wall, current[OPPOSITE[n]], moved)
    return density, post


def streamed(n, x, post, low, high, scales=None):
    vx, vy, vz = VELOCITIES[n]
    source = x + 1 - vx
    cy, nz = post.shape[2:]
    yrow = lax.broadcasted_iota(jnp.int32, (cy, nz), 0)
    value = post[SLOT[n], source]
    if scales:
        scale, scale_low, scale_high = [ref[(source + TILE - 1) // TILE] for ref in scales]
        value = value * scale
    if vy == 1:
        edge = low[RISING_Y.index(n), source]
        edge = edge * scale_low if scales else edge
        value = jnp.where(yrow == 0, edge, pltpu.roll(value, 1, 0))
    elif vy == -1:
        edge = high[FALLING_Y.index(n), source]
        edge = edge * scale_high if scales else edge
        value = jnp.where(yrow == cy - 1, edge, pltpu.roll(value, cy - 1, 0))
    if vz:
        value = pltpu.roll(value, vz % nz, 1)
    return value


def finish(post, low, high, means, out_hbm, means_out, out_ref, sems):
    means_out[...] = means[...]
    copies = []
    for n in range(19):
        for x in range(out_ref.shape[1]):
            out_ref[n, x] = streamed(n, x, post, low, high)
        copies.append(pltpu.make_async_copy(out_ref.at[n], out_hbm.at[n], sems.at[n]))
        copies[-1].start()
    for copy in copies:
        copy.wait()


def kernel(
    ngx,
    ngy,
    cx,
    cy,
    region_hbm,
    pops_hbm,
    kind_hbm,
    post_b,
    low_b,
    high_b,
    means_ref,
    region_ref,
    pops_ref,
    kind_ref,
    load_sems,
    post_a,
    density_ref,
    up_a,
    down_a,
    up_b,
    down_b,
    low_a,
    high_a,
    row_ref,
    table,
    spread,
    mult,
    mult_low,
    mult_high,
    send_sems,
    recv_sems,
    gather_sems,
):
    gx = lax.axis_index("gx")
    gy = lax.axis_index("gy")
    count = ngx * ngy
    me = gx * ngy + gy
    tx_n, ty_n = cx // TILE, cy // TILE
    nz = pops_ref.shape[3]
    lane = lax.broadcasted_iota(jnp.int32, (1, 128), 1)
    zlane = lax.broadcasted_iota(jnp.int32, (cy, nz), 1)
    yrow = lax.broadcasted_iota(jnp.int32, (cy, nz), 0)

    loads = [
        pltpu.make_async_copy(region_hbm, region_ref, load_sems.at[2]),
        pltpu.make_async_copy(pops_hbm, pops_ref, load_sems.at[0]),
        pltpu.make_async_copy(kind_hbm, kind_ref, load_sems.at[1]),
    ]
    for load in loads:
        load.start()
    barrier = pltpu.get_barrier_semaphore()

    def wrapped(value, size):
        return jnp.where(value >= size, value - size, value)

    def every_peer(visit):
        for ox in range(ngx):
            px = wrapped(gx + ox, ngx)

            def one(oy, carry):
                visit({"gx": px, "gy": wrapped(gy + oy, ngy)})
                return carry

            lax.fori_loop(0 if ox else 1, ngy, one, 0, unroll=ngy <= 8)

    every_peer(
        lambda peer: pl.semaphore_signal(barrier, inc=1, device_id=peer, device_id_type=MESH)
    )

    def first(x, carry):
        current = [pops_ref[n, x] for n in range(19)]
        density, post = collide(current, kind_ref[x], 1.0)
        density_ref[x] = density
        for n in range(19):
            post_a[SLOT[n], x + 1] = post[n]
        for k in range(5):
            up_a[k, x] = post[RISING_Y[k]][cy - 1 :, :]
            down_a[k, x] = post[FALLING_Y[k]][:1, :]
        return carry

    for load in loads:
        load.wait()
    lax.fori_loop(0, cx, first, 0)

    sums = {}

    def put(key, value):
        sums[key] = value if key not in sums else sums[key] + value

    for tx in range(tx_n):
        for i in range(TILE):
            x = tx * TILE + i
            for vx in (-1, 0, 1):
                dx = vx if (vx == 1 and i == TILE - 1) or (vx == -1 and i == 0) else 0
                for vy in (-1, 0, 1):
                    flat = jnp.where(
                        zlane == nz - 1, post_a[SLOT[NUMBER[(vx, vy, 0)]], x + 1], 0.0
                    )
                    if (vx, vy, 1) in NUMBER:
                        rising = post_a[SLOT[NUMBER[(vx, vy, 1)]], x + 1]
                        falling = post_a[SLOT[NUMBER[(vx, vy, -1)]], x + 1]
                        flat = jnp.where(zlane == nz - 2, rising, flat)
                        flat = jnp.where(zlane == 0, falling, flat)
                    put((tx, dx, vy), flat)
            put((tx, "rho"), jnp.where(zlane == nz - 1, density_ref[x], 0.0))
    stage = jnp.zeros((cy, 128), jnp.float32)
    lane8 = lax.broadcasted_iota(jnp.int32, (cy, 128), 1)
    row8 = lax.broadcasted_iota(jnp.int32, (cy, 128), 0)
    block = 16 * ty_n
    for tx in range(tx_n):
        for dx in (-1, 0, 1):
            for vy in (-1, 0, 1):
                value = sums[(tx, dx, vy)]
                fixed = jnp.sum(jnp.where(zlane == nz - 1, 0.0, value), axis=1, keepdims=True)
                scaled = jnp.sum(jnp.where(zlane == nz - 1, value, 0.0), axis=1, keepdims=True)
                at = tx * block + (dx + 1) * 4 + vy + 1
                stage = jnp.where(lane8 == at, fixed, stage)
                stage = jnp.where(lane8 == 64 + at, scaled, stage)
        rho = jnp.sum(sums[(tx, "rho")], axis=1, keepdims=True)
        stage = jnp.where(lane8 == tx * block + 13, rho, stage)
    slot8 = lane8 & 3
    message = jnp.zeros((1, 128), jnp.float32)
    for ty in range(ty_n):
        first_row, last_row = ty * TILE, ty * TILE + TILE - 1
        inside = (row8 >= first_row) & (row8 <= last_row)
        crossing = ((slot8 == 2) & (row8 == last_row)) | ((slot8 == 0) & (row8 == first_row))
        cross = jnp.sum(jnp.where(crossing, stage, 0.0), axis=0, keepdims=True)
        stay = jnp.where(inside & jnp.logical_not(crossing), stage, 0.0)
        stay = jnp.broadcast_to(jnp.sum(stay, axis=0, keepdims=True), (8, 128))
        stay = (stay + pltpu.roll(stay, 1, 1) + pltpu.roll(stay, 127, 1))[:1]
        both = jnp.where((lane & 3) == 1, stay, cross)
        if ty:
            both = pltpu.roll(jnp.broadcast_to(both, (8, 128)), 16 * ty, 1)[:1]
        message = message + both
    for tx in range(tx_n):
        for ty in range(ty_n):
            region = region_ref[tx * TILE, ty * TILE].astype(jnp.float32)
            message = jnp.where(lane == 64 + tx * block + ty * 16 + 13, region, message)
    row_ref[...] = message
    table[me] = message

    pl.semaphore_wait(barrier, count - 1)

    every_peer(
        lambda peer: pltpu.make_async_remote_copy(
            src_ref=row_ref,
            dst_ref=table.at[me],
            send_sem=gather_sems.at[0],
            recv_sem=gather_sems.at[1],
            device_id=peer,
            device_id_type=MESH,
        ).start()
    )

    def exchange(step, post, up, down, low, high):
        def send(k, source, target, ox, oy):
            copy = pltpu.make_async_remote_copy(
                src_ref=source,
                dst_ref=target,
                send_sem=send_sems.at[step, k],
                recv_sem=recv_sems.at[step, k],
                device_id={"gx": lax.rem(gx + ox + ngx, ngx), "gy": lax.rem(gy + oy + ngy, ngy)},
                device_id_type=MESH,
            )
            copy.start()
            return copy

        return [
            send(0, up.at[RISING_Y.index(7), cx - 1], low.at[RISING_Y.index(7), 0], 1, 1),
            send(1, up.at[RISING_Y.index(10), 0], low.at[RISING_Y.index(10), cx + 1], -1, 1),
            send(2, down.at[FALLING_Y.index(9), cx - 1], high.at[FALLING_Y.index(9), 0], 1, -1),
            send(3, down.at[FALLING_Y.index(8), 0], high.at[FALLING_Y.index(8), cx + 1], -1, -1),
            send(4, up, low.at[:, pl.ds(1, cx)], 0, 1),
            send(5, down, high.at[:, pl.ds(1, cx)], 0, -1),
            send(6, post.at[pl.ds(0, 5), cx], post.at[pl.ds(0, 5), 0], 1, 0),
            send(7, post.at[pl.ds(5, 5), 1], post.at[pl.ds(5, 5), cx + 1], -1, 0),
        ]

    def rims(post, low, high):
        @pl.when(gx == 0)
        def _():
            post[0:5, 0] = jnp.zeros((5, cy, nz), jnp.float32)
            low[RISING_Y.index(7), 0] = jnp.zeros((1, nz), jnp.float32)
            high[FALLING_Y.index(9), 0] = jnp.zeros((1, nz), jnp.float32)

        @pl.when(gx == ngx - 1)
        def _():
            post[5:10, cx + 1] = jnp.zeros((5, cy, nz), jnp.float32)
            low[RISING_Y.index(10), cx + 1] = jnp.zeros((1, nz), jnp.float32)
            high[FALLING_Y.index(8), cx + 1] = jnp.zeros((1, nz), jnp.float32)

    copies = exchange(0, post_a, up_a, down_a, low_a, high_a)

    whole = pltpu.make_async_copy(
        table.at[pl.ds(0, count - 1)], table.at[pl.ds(0, count - 1)], gather_sems.at[1]
    )
    whole.wait()
    pltpu.make_async_copy(
        table.at[pl.ds(0, count - 1)], table.at[pl.ds(0, count - 1)], gather_sems.at[0]
    ).wait()

    tiles = tx_n * ty_n
    lanes = lax.broadcasted_iota(jnp.int32, (ngy, 128), 1)
    lanes_f = lanes.astype(jnp.float32)
    rows = [table[pl.ds(X * ngy, ngy), 0, :] for X in range(ngx)]
    onehot = {}
    total = jnp.zeros((ngy, 128), jnp.float32)
    cells = jnp.zeros((ngy, 128), jnp.float32)
    for X in range(ngx):
        for q in range(tiles):
            at = q * 16 + 13
            onehot[X, q] = rows[X][:, 64 + at : 65 + at] == lanes_f
            total = total + jnp.where(onehot[X, q], rows[X][:, at : at + 1], 0.0)
            cells = cells + jnp.where(onehot[X, q], 1.0 * TILE * TILE, 0.0)
    cells = jnp.sum(cells, axis=0, keepdims=True)
    cells = jnp.where(cells > 0.0, cells, 1.0)
    mean_1 = jnp.sum(total, axis=0, keepdims=True) / cells
    means_ref[0:1, :] = mean_1[:, :REGIONS]

    tile_x, tile_y = (lanes >> 4) // ty_n, (lanes >> 4) % ty_n
    step_x, step_y = ((lanes >> 2) & 3) - 1, (lanes & 3) - 1
    real = (lanes < 16 * tiles) & (step_x < 2) & (step_y < 2)
    to_x, to_y = tile_x + step_x, tile_y + step_y
    off_x = jnp.where(to_x < 0, -1, jnp.where(to_x >= tx_n, 1, 0))
    off_y = jnp.where(to_y < 0, -1, jnp.where(to_y >= ty_n, 1, 0))
    goal = (to_x - off_x * tx_n) * ty_n + (to_y - off_y * ty_n)
    shifted = []
    for X in range(ngx):
        by_tile = jnp.zeros((ngy, 128), jnp.float32)
        for q in range(tiles):
            m = jnp.sum(jnp.where(onehot[X, q], mean_1, 0.0), axis=1, keepdims=True)
            by_tile = jnp.where((lanes >> 4) == q, m, by_tile)
        spread[X] = by_tile
        value = jnp.where(real, rows[X] + by_tile * pltpu.roll(rows[X], 64, 1), 0.0)
        moved = jnp.where(off_y == 0, value, 0.0)
        moved = moved + pltpu.roll(jnp.where(off_y == 1, value, 0.0), 1, 0)
        moved = moved + pltpu.roll(jnp.where(off_y == -1, value, 0.0), ngy - 1, 0)
        shifted.append(moved)
    total = jnp.zeros((ngy, 128), jnp.float32)
    for X in range(ngx):
        landed = jnp.where(off_x == 0, shifted[X], 0.0)
        if X > 0:
            landed = landed + jnp.where(off_x == 1, shifted[X - 1], 0.0)
        if X < ngx - 1:
            landed = landed + jnp.where(off_x == -1, shifted[X + 1], 0.0)
        for q in range(tiles):
            s = jnp.sum(jnp.where(goal == q, landed, 0.0), axis=1, keepdims=True)
            total = total + jnp.where(onehot[X, q], s, 0.0)
    mean_2 = jnp.sum(total, axis=0, keepdims=True) / cells
    means_ref[1:2, :] = mean_2[:, :REGIONS]

    around = {}
    for ox in (-1, 0, 1):
        for oy in (-1, 0, 1):
            sx = jnp.clip(gx + ox, 0, ngx - 1)
            sy = lax.rem(gy + oy + ngy, ngy)
            around[ox, oy] = spread[sx, pl.ds(sy, 1), :]

    def tile_mean(tx, ty):
        ox = -1 if tx < 0 else 1 if tx >= tx_n else 0
        oy = -1 if ty < 0 else 1 if ty >= ty_n else 0
        at = ((tx - ox * tx_n) * ty_n + ty - oy * ty_n) * 16
        return around[ox, oy][:, at : at + 1]

    def columns(values):
        result = values[0]
        for ty in range(1, ty_n):
            result = jnp.where(yrow >= ty * TILE, values[ty], result)
        return result

    zrow = lax.broadcasted_iota(jnp.int32, (1, nz), 1)
    for k in range(tx_n + 2):
        mult[k] = jnp.where(
            zlane == nz - 1, columns([tile_mean(k - 1, ty) for ty in range(ty_n)]), 1.0
        )
        mult_low[k] = jnp.where(zrow == nz - 1, tile_mean(k - 1, -1), 1.0)
        mult_high[k] = jnp.where(zrow == nz - 1, tile_mean(k - 1, ty_n), 1.0)
    outlet_2 = []
    for tx in range(tx_n):
        values = []
        for ty in range(ty_n):
            mine = lane == region_ref[tx * TILE, ty * TILE]
            values.append(jnp.sum(jnp.where(mine, mean_2, 0.0), axis=1, keepdims=True))
        outlet_2.append(columns(values) + jnp.zeros((cy, nz), jnp.float32))

    for copy in copies:
        copy.wait()
    rims(post_a, low_a, high_a)

    for tx in range(tx_n):

        def second(x, carry):
            current = [streamed(n, x, post_a, low_a, high_a, (mult, mult_low, mult_high)) for n in range(19)]
            _, post = collide(current, kind_ref[x], outlet_2[tx])
            for n in range(19):
                post_b[SLOT[n], x + 1] = post[n]
            for k in range(5):
                up_b[k, x] = post[RISING_Y[k]][cy - 1 :, :]
                down_b[k, x] = post[FALLING_Y[k]][:1, :]
            return carry

        lax.fori_loop(tx * TILE, tx * TILE + TILE, second, 0)

    copies = exchange(1, post_b, up_b, down_b, low_b, high_b)
    for copy in copies:
        copy.wait()
    rims(post_b, low_b, high_b)


def solution(mesh):
    ngx, ngy = mesh.shape["gx"], mesh.shape["gy"]

    def body(populations, cell_kind, outlet_region):
        _, cx, cy, nz = populations.shape
        f32 = jnp.float32
        arrays = (outlet_region, populations, cell_kind)
        vmem = pl.BlockSpec(memory_space=pltpu.VMEM)
        hbm = pl.BlockSpec(memory_space=pltpu.HBM)
        middle = pl.pallas_call(
            functools.partial(kernel, ngx, ngy, cx, cy),
            out_shape=(
                pltpu.VMEM((19, cx + 2, cy, nz), f32),
                pltpu.VMEM((5, cx + 2, 1, nz), f32),
                pltpu.VMEM((5, cx + 2, 1, nz), f32),
                pltpu.VMEM((2, REGIONS), f32),
            ),
            in_specs=[hbm, hbm, hbm],
            out_specs=(vmem, vmem, vmem, vmem),
            scratch_shapes=[
                pltpu.SMEM(outlet_region.shape, jnp.int32),
                pltpu.VMEM(populations.shape, f32),
                pltpu.VMEM(cell_kind.shape, jnp.int32),
                pltpu.SemaphoreType.DMA((3,)),
                pltpu.VMEM((19, cx + 2, cy, nz), f32),
                pltpu.VMEM((cx, cy, nz), f32),
                pltpu.VMEM((5, cx, 1, nz), f32),
                pltpu.VMEM((5, cx, 1, nz), f32),
                pltpu.VMEM((5, cx, 1, nz), f32),
                pltpu.VMEM((5, cx, 1, nz), f32),
                pltpu.VMEM((5, cx + 2, 1, nz), f32),
                pltpu.VMEM((5, cx + 2, 1, nz), f32),
                pltpu.VMEM((1, 128), f32),
                pltpu.VMEM((ngx * ngy, 1, 128), f32),
                pltpu.VMEM((ngx, ngy, 128), f32),
                pltpu.VMEM((cx // TILE + 2, cy, nz), f32),
                pltpu.VMEM((cx // TILE + 2, 1, nz), f32),
                pltpu.VMEM((cx // TILE + 2, 1, nz), f32),
                pltpu.SemaphoreType.DMA((2, 8)),
                pltpu.SemaphoreType.DMA((2, 8)),
                pltpu.SemaphoreType.DMA((2,)),
            ],
            compiler_params=pltpu.CompilerParams(
                collective_id=0, has_side_effects=True, vmem_limit_bytes=48 * 2**20
            ),
        )(*[pltpu.with_memory_space_constraint(a, pltpu.HBM) for a in arrays])
        return pl.pallas_call(
            finish,
            out_shape=(
                jax.ShapeDtypeStruct(populations.shape, f32),
                jax.ShapeDtypeStruct((2, REGIONS), f32),
            ),
            in_specs=[vmem, vmem, vmem, vmem],
            out_specs=(hbm, vmem),
            scratch_shapes=[
                pltpu.VMEM(populations.shape, f32),
                pltpu.SemaphoreType.DMA((19,)),
            ],
            compiler_params=pltpu.CompilerParams(vmem_limit_bytes=16 * 2**20),
        )(*middle)

    in_specs = (P(None, "gx", "gy", None), P("gx", "gy", None), P("gx", "gy"))
    out_specs = (P(None, "gx", "gy", None), P())
    return jax.shard_map(body, mesh=mesh, in_specs=in_specs, out_specs=out_specs, check_vma=False)
```

```python
import functools

import jax
import jax.numpy as jnp
from jax import lax
from jax.experimental import pallas as pl
from jax.experimental.pallas import tpu as pltpu
from jax.sharding import PartitionSpec as P

REGIONS = 64
TILE = 4
VELOCITIES = (
    (0, 0, 0),
    (1, 0, 0),
    (-1, 0, 0),
    (0, 1, 0),
    (0, -1, 0),
    (0, 0, 1),
    (0, 0, -1),
    (1, 1, 0),
    (-1, -1, 0),
    (1, -1, 0),
    (-1, 1, 0),
    (1, 0, 1),
    (-1, 0, -1),
    (1, 0, -1),
    (-1, 0, 1),
    (0, 1, 1),
    (0, -1, -1),
    (0, 1, -1),
    (0, -1, 1),
)
NUMBER = {velocity: number for number, velocity in enumerate(VELOCITIES)}
WEIGHTS = (1.0 / 3.0,) + (1.0 / 18.0,) * 6 + (1.0 / 36.0,) * 12
OPPOSITE = (0, 2, 1, 4, 3, 6, 5, 8, 7, 10, 9, 12, 11, 14, 13, 16, 15, 18, 17)
RELAX_TIME = 0.8
INLET_SPEED = 0.05
RISING_X = (1, 7, 9, 11, 13)
FALLING_X = (2, 8, 10, 12, 14)
RISING_Y = (3, 7, 10, 15, 17)
FALLING_Y = (4, 8, 9, 16, 18)
SLOTS = RISING_X + FALLING_X + (0, 3, 4, 5, 6, 15, 16, 17, 18)
SLOT = {number: slot for slot, number in enumerate(SLOTS)}
MESH = pl.DeviceIdType.MESH


def inlet_value(number):
    comp_z = VELOCITIES[number][2]
    projected = comp_z * INLET_SPEED
    return WEIGHTS[number] * (
        1.0 + 3.0 * projected + 4.5 * projected * projected - 1.5 * INLET_SPEED * INLET_SPEED
    )


def signed_sum(terms):
    total = None
    for sign, value in terms:
        if total is None:
            total = value if sign > 0 else -value
        else:
            total = total + value if sign > 0 else total - value
    return total


def collide(current, kinds, outlet_density):
    density = functools.reduce(lambda a, b: a + b, current)
    inverse = 1.0 / density
    vel = [
        signed_sum([(v[d], current[n]) for n, v in enumerate(VELOCITIES) if v[d] != 0]) * inverse
        for d in range(3)
    ]
    base = 1.0 - 1.5 * (vel[0] * vel[0] + vel[1] * vel[1] + vel[2] * vel[2])
    wall = kinds == 1
    inlet = kinds == 2
    outlet = kinds == 3
    keep = jnp.where(outlet, 0.0, 1.0 - 1.0 / RELAX_TIME)
    scale = jnp.where(outlet, outlet_density, density * (1.0 / RELAX_TIME))
    scales = {w: scale * w for w in sorted(set(WEIGHTS))}
    post = [None] * 19
    for number in range(19):
        if number > OPPOSITE[number]:
            continue
        other = OPPOSITE[number]
        if number == 0:
            pairs = ((0, base),)
        else:
            projected = signed_sum([(c, vel[d]) for d, c in enumerate(VELOCITIES[number]) if c])
            even = base + 4.5 * projected * projected
            odd = 3.0 * projected
            pairs = ((number, even + odd), (other, even - odd))
        for n, unit in pairs:
            moved = keep * current[n] + scales[WEIGHTS[n]] * unit
            moved = jnp.where(inlet, inlet_value(n), moved)
            post[n] = jnp.where(wall, current[OPPOSITE[n]], moved)
    return density, post


def streamed(n, x, post, low, high, scales=None):
    vx, vy, vz = VELOCITIES[n]
    source = x + 1 - vx
    cy, nz = post.shape[2:]
    yrow = lax.broadcasted_iota(jnp.int32, (cy, nz), 0)
    value = post[SLOT[n], source]
    if scales:
        scale, scale_low, scale_high = [ref[(source + TILE - 1) // TILE] for ref in scales]
        value = value * scale
    if vy == 1:
        edge = low[RISING_Y.index(n), source]
        edge = edge * scale_low if scales else edge
        value = jnp.where(yrow == 0, edge, pltpu.roll(value, 1, 0))
    elif vy == -1:
        edge = high[FALLING_Y.index(n), source]
        edge = edge * scale_high if scales else edge
        value = jnp.where(yrow == cy - 1, edge, pltpu.roll(value, cy - 1, 0))
    if vz:
        value = pltpu.roll(value, vz % nz, 1)
    return value


def finish(post, low, high, means, mult, mult_low, mult_high, out_hbm, means_out, out_ref, sems):
    means_out[...] = means[...]
    copies = []
    for n in range(19):
        for x in range(out_ref.shape[1]):
            out_ref[n, x] = streamed(n, x, post, low, high, (mult, mult_low, mult_high))
        copies.append(pltpu.make_async_copy(out_ref.at[n], out_hbm.at[n], sems.at[n]))
        copies[-1].start()
    for copy in copies:
        copy.wait()


def kernel(
    ngx,
    ngy,
    cx,
    cy,
    region_hbm,
    pops_hbm,
    kind_hbm,
    post_b,
    low_b,
    high_b,
    means_ref,
    mult_b,
    mult_low_b,
    mult_high_b,
    region_ref,
    pops_ref,
    kind_ref,
    load_sems,
    post_a,
    density_ref,
    up_a,
    down_a,
    up_b,
    down_b,
    low_a,
    high_a,
    row_ref,
    table,
    spread,
    mult,
    mult_low,
    mult_high,
    send_sems,
    recv_sems,
    gather_sems,
):
    gx = lax.axis_index("gx")
    gy = lax.axis_index("gy")
    count = ngx * ngy
    me = gx * ngy + gy
    tx_n, ty_n = cx // TILE, cy // TILE
    nz = pops_ref.shape[3]
    lane = lax.broadcasted_iota(jnp.int32, (1, 128), 1)
    zlane = lax.broadcasted_iota(jnp.int32, (cy, nz), 1)
    yrow = lax.broadcasted_iota(jnp.int32, (cy, nz), 0)

    loads = [
        pltpu.make_async_copy(region_hbm, region_ref, load_sems.at[2]),
        pltpu.make_async_copy(pops_hbm, pops_ref, load_sems.at[0]),
        pltpu.make_async_copy(kind_hbm, kind_ref, load_sems.at[1]),
    ]
    for load in loads:
        load.start()
    barrier = pltpu.get_barrier_semaphore()

    def wrapped(value, size):
        return jnp.where(value >= size, value - size, value)

    def every_peer(visit):
        for turn in range(ngy):
            away = ngy - (turn + 1) // 2 if turn % 2 else turn // 2
            py = wrapped(ngy - 1 - gy + away, ngy)

            def one(ox, carry):
                visit({"gx": wrapped(gx + ox, ngx), "gy": py})
                return carry

            @pl.when(py != gy)
            def _():
                visit({"gx": gx, "gy": py})

            lax.fori_loop(1, ngx, one, 0, unroll=ngx <= 4)

    every_peer(
        lambda peer: pl.semaphore_signal(barrier, inc=1, device_id=peer, device_id_type=MESH)
    )

    def first(x, carry):
        current = [pops_ref[n, x] for n in range(19)]
        density, post = collide(current, kind_ref[x], 1.0)
        density_ref[x] = density
        for n in range(19):
            post_a[SLOT[n], x + 1] = post[n]
        for k in range(5):
            up_a[k, x] = post[RISING_Y[k]][cy - 1 :, :]
            down_a[k, x] = post[FALLING_Y[k]][:1, :]
        return carry

    for load in loads:
        load.wait()
    lax.fori_loop(0, cx, first, 0)

    sums = {}

    def put(key, value):
        sums[key] = value if key not in sums else sums[key] + value

    for tx in range(tx_n):
        for i in range(TILE):
            x = tx * TILE + i
            for vx in (-1, 0, 1):
                dx = vx if (vx == 1 and i == TILE - 1) or (vx == -1 and i == 0) else 0
                for vy in (-1, 0, 1):
                    flat = jnp.where(
                        zlane == nz - 1, post_a[SLOT[NUMBER[(vx, vy, 0)]], x + 1], 0.0
                    )
                    if (vx, vy, 1) in NUMBER:
                        rising = post_a[SLOT[NUMBER[(vx, vy, 1)]], x + 1]
                        falling = post_a[SLOT[NUMBER[(vx, vy, -1)]], x + 1]
                        flat = jnp.where(zlane == nz - 2, rising, flat)
                        flat = jnp.where(zlane == 0, falling, flat)
                    put((tx, dx, vy), flat)
            put((tx, "rho"), jnp.where(zlane == nz - 1, density_ref[x], 0.0))
    stage = jnp.zeros((cy, 128), jnp.float32)
    lane8 = lax.broadcasted_iota(jnp.int32, (cy, 128), 1)
    row8 = lax.broadcasted_iota(jnp.int32, (cy, 128), 0)
    block = 16 * ty_n
    for tx in range(tx_n):
        for dx in (-1, 0, 1):
            for vy in (-1, 0, 1):
                value = sums[(tx, dx, vy)]
                fixed = jnp.sum(jnp.where(zlane == nz - 1, 0.0, value), axis=1, keepdims=True)
                scaled = jnp.sum(jnp.where(zlane == nz - 1, value, 0.0), axis=1, keepdims=True)
                at = tx * block + (dx + 1) * 4 + vy + 1
                stage = jnp.where(lane8 == at, fixed, stage)
                stage = jnp.where(lane8 == 64 + at, scaled, stage)
        rho = jnp.sum(sums[(tx, "rho")], axis=1, keepdims=True)
        stage = jnp.where(lane8 == tx * block + 13, rho, stage)
    slot8 = lane8 & 3
    message = jnp.zeros((1, 128), jnp.float32)
    for ty in range(ty_n):
        first_row, last_row = ty * TILE, ty * TILE + TILE - 1
        inside = (row8 >= first_row) & (row8 <= last_row)
        crossing = ((slot8 == 2) & (row8 == last_row)) | ((slot8 == 0) & (row8 == first_row))
        cross = jnp.sum(jnp.where(crossing, stage, 0.0), axis=0, keepdims=True)
        stay = jnp.where(inside & jnp.logical_not(crossing), stage, 0.0)
        stay = jnp.broadcast_to(jnp.sum(stay, axis=0, keepdims=True), (8, 128))
        stay = (stay + pltpu.roll(stay, 1, 1) + pltpu.roll(stay, 127, 1))[:1]
        both = jnp.where((lane & 3) == 1, stay, cross)
        if ty:
            both = pltpu.roll(jnp.broadcast_to(both, (8, 128)), 16 * ty, 1)[:1]
        message = message + both
    for tx in range(tx_n):
        for ty in range(ty_n):
            region = region_ref[tx * TILE, ty * TILE].astype(jnp.float32)
            message = jnp.where(lane == 64 + tx * block + ty * 16 + 13, region, message)
    row_ref[...] = message
    table[me] = message

    pl.semaphore_wait(barrier, count - 1)

    every_peer(
        lambda peer: pltpu.make_async_remote_copy(
            src_ref=row_ref,
            dst_ref=table.at[me],
            send_sem=gather_sems.at[0],
            recv_sem=gather_sems.at[1],
            device_id=peer,
            device_id_type=MESH,
        ).start()
    )

    def exchange(step, post, up, down, low, high):
        def send(k, source, target, ox, oy):
            copy = pltpu.make_async_remote_copy(
                src_ref=source,
                dst_ref=target,
                send_sem=send_sems.at[step, k],
                recv_sem=recv_sems.at[step, k],
                device_id={"gx": lax.rem(gx + ox + ngx, ngx), "gy": lax.rem(gy + oy + ngy, ngy)},
                device_id_type=MESH,
            )
            copy.start()
            return copy

        return [
            send(0, up.at[RISING_Y.index(7), cx - 1], low.at[RISING_Y.index(7), 0], 1, 1),
            send(1, up.at[RISING_Y.index(10), 0], low.at[RISING_Y.index(10), cx + 1], -1, 1),
            send(2, down.at[FALLING_Y.index(9), cx - 1], high.at[FALLING_Y.index(9), 0], 1, -1),
            send(3, down.at[FALLING_Y.index(8), 0], high.at[FALLING_Y.index(8), cx + 1], -1, -1),
            send(4, up, low.at[:, pl.ds(1, cx)], 0, 1),
            send(5, down, high.at[:, pl.ds(1, cx)], 0, -1),
            send(6, post.at[pl.ds(0, 5), cx], post.at[pl.ds(0, 5), 0], 1, 0),
            send(7, post.at[pl.ds(5, 5), 1], post.at[pl.ds(5, 5), cx + 1], -1, 0),
        ]

    def rims(post, low, high):
        @pl.when(gx == 0)
        def _():
            post[0:5, 0] = jnp.zeros((5, cy, nz), jnp.float32)
            low[RISING_Y.index(7), 0] = jnp.zeros((1, nz), jnp.float32)
            high[FALLING_Y.index(9), 0] = jnp.zeros((1, nz), jnp.float32)

        @pl.when(gx == ngx - 1)
        def _():
            post[5:10, cx + 1] = jnp.zeros((5, cy, nz), jnp.float32)
            low[RISING_Y.index(10), cx + 1] = jnp.zeros((1, nz), jnp.float32)
            high[FALLING_Y.index(8), cx + 1] = jnp.zeros((1, nz), jnp.float32)

    copies = exchange(0, post_a, up_a, down_a, low_a, high_a)

    whole = pltpu.make_async_copy(
        table.at[pl.ds(0, count - 1)], table.at[pl.ds(0, count - 1)], gather_sems.at[1]
    )
    whole.wait()
    pltpu.make_async_copy(
        table.at[pl.ds(0, count - 1)], table.at[pl.ds(0, count - 1)], gather_sems.at[0]
    ).wait()

    tiles = tx_n * ty_n
    lanes = lax.broadcasted_iota(jnp.int32, (ngy, 128), 1)
    lanes_f = lanes.astype(jnp.float32)
    rows = [table[pl.ds(X * ngy, ngy), 0, :] for X in range(ngx)]
    onehot = {}
    total = jnp.zeros((ngy, 128), jnp.float32)
    cells = jnp.zeros((ngy, 128), jnp.float32)
    for X in range(ngx):
        for q in range(tiles):
            at = q * 16 + 13
            onehot[X, q] = rows[X][:, 64 + at : 65 + at] == lanes_f
            total = total + jnp.where(onehot[X, q], rows[X][:, at : at + 1], 0.0)
            cells = cells + jnp.where(onehot[X, q], 1.0 * TILE * TILE, 0.0)
    cells = jnp.sum(cells, axis=0, keepdims=True)
    cells = jnp.where(cells > 0.0, cells, 1.0)
    mean_1 = jnp.sum(total, axis=0, keepdims=True) / cells
    means_ref[0:1, :] = mean_1[:, :REGIONS]

    def by_region(mean, X):
        result = jnp.zeros((ngy, 128), jnp.float32)
        for q in range(tiles):
            m = jnp.sum(jnp.where(onehot[X, q], mean, 0.0), axis=1, keepdims=True)
            result = jnp.where((lanes >> 4) == q, m, result)
        return result

    by_tile = [by_region(mean_1, X) for X in range(ngx)]
    for X in range(ngx):
        spread[0, X] = by_tile[X]

    zrow = lax.broadcasted_iota(jnp.int32, (1, nz), 1)

    def scale_outlets(step, mult, mult_low, mult_high):
        around = {}
        for ox in (-1, 0, 1):
            for oy in (-1, 0, 1):
                sx = jnp.clip(gx + ox, 0, ngx - 1)
                sy = lax.rem(gy + oy + ngy, ngy)
                around[ox, oy] = spread[step, sx, pl.ds(sy, 1), :]

        def tile_mean(tx, ty):
            ox = -1 if tx < 0 else 1 if tx >= tx_n else 0
            oy = -1 if ty < 0 else 1 if ty >= ty_n else 0
            at = ((tx - ox * tx_n) * ty_n + ty - oy * ty_n) * 16
            return around[ox, oy][:, at : at + 1]

        for k in range(tx_n + 2):
            column = tile_mean(k - 1, 0)
            for ty in range(1, ty_n):
                column = jnp.where(yrow >= ty * TILE, tile_mean(k - 1, ty), column)
            mult[k] = jnp.where(zlane == nz - 1, column, 1.0)
            mult_low[k] = jnp.where(zrow == nz - 1, tile_mean(k - 1, -1), 1.0)
            mult_high[k] = jnp.where(zrow == nz - 1, tile_mean(k - 1, ty_n), 1.0)

    scale_outlets(0, mult, mult_low, mult_high)

    for copy in copies:
        copy.wait()
    rims(post_a, low_a, high_a)

    def second(x, carry):
        current = [
            streamed(n, x, post_a, low_a, high_a, (mult, mult_low, mult_high)) for n in range(19)
        ]
        _, post = collide(current, kind_ref[x], 1.0)
        for n in range(19):
            post_b[SLOT[n], x + 1] = post[n]
        for k in range(5):
            up_b[k, x] = post[RISING_Y[k]][cy - 1 :, :]
            down_b[k, x] = post[FALLING_Y[k]][:1, :]
        return carry

    lax.fori_loop(0, cx, second, 0)

    copies = exchange(1, post_b, up_b, down_b, low_b, high_b)

    tile_x, tile_y = (lanes >> 4) // ty_n, (lanes >> 4) % ty_n
    step_x, step_y = ((lanes >> 2) & 3) - 1, (lanes & 3) - 1
    real = (lanes < 16 * tiles) & (step_x < 2) & (step_y < 2)
    to_x, to_y = tile_x + step_x, tile_y + step_y
    off_x = jnp.where(to_x < 0, -1, jnp.where(to_x >= tx_n, 1, 0))
    off_y = jnp.where(to_y < 0, -1, jnp.where(to_y >= ty_n, 1, 0))
    goal = (to_x - off_x * tx_n) * ty_n + (to_y - off_y * ty_n)
    shifted = []
    for X in range(ngx):
        value = jnp.where(real, rows[X] + by_tile[X] * pltpu.roll(rows[X], 64, 1), 0.0)
        moved = jnp.where(off_y == 0, value, 0.0)
        moved = moved + pltpu.roll(jnp.where(off_y == 1, value, 0.0), 1, 0)
        moved = moved + pltpu.roll(jnp.where(off_y == -1, value, 0.0), ngy - 1, 0)
        shifted.append(moved)
    total = jnp.zeros((ngy, 128), jnp.float32)
    for X in range(ngx):
        landed = jnp.where(off_x == 0, shifted[X], 0.0)
        if X > 0:
            landed = landed + jnp.where(off_x == 1, shifted[X - 1], 0.0)
        if X < ngx - 1:
            landed = landed + jnp.where(off_x == -1, shifted[X + 1], 0.0)
        for q in range(tiles):
            s = jnp.sum(jnp.where(goal == q, landed, 0.0), axis=1, keepdims=True)
            total = total + jnp.where(onehot[X, q], s, 0.0)
    mean_2 = jnp.sum(total, axis=0, keepdims=True) / cells
    means_ref[1:2, :] = mean_2[:, :REGIONS]

    for X in range(ngx):
        spread[1, X] = by_region(mean_2, X)
    scale_outlets(1, mult_b, mult_low_b, mult_high_b)

    for copy in copies:
        copy.wait()
    rims(post_b, low_b, high_b)


def solution(mesh):
    ngx, ngy = mesh.shape["gx"], mesh.shape["gy"]

    def body(populations, cell_kind, outlet_region):
        _, cx, cy, nz = populations.shape
        f32 = jnp.float32
        arrays = (outlet_region, populations, cell_kind)
        vmem = pl.BlockSpec(memory_space=pltpu.VMEM)
        hbm = pl.BlockSpec(memory_space=pltpu.HBM)
        middle = pl.pallas_call(
            functools.partial(kernel, ngx, ngy, cx, cy),
            out_shape=(
                pltpu.VMEM((19, cx + 2, cy, nz), f32),
                pltpu.VMEM((5, cx + 2, 1, nz), f32),
                pltpu.VMEM((5, cx + 2, 1, nz), f32),
                pltpu.VMEM((2, REGIONS), f32),
                pltpu.VMEM((cx // TILE + 2, cy, nz), f32),
                pltpu.VMEM((cx // TILE + 2, 1, nz), f32),
                pltpu.VMEM((cx // TILE + 2, 1, nz), f32),
            ),
            in_specs=[hbm, hbm, hbm],
            out_specs=(vmem,) * 7,
            scratch_shapes=[
                pltpu.SMEM(outlet_region.shape, jnp.int32),
                pltpu.VMEM(populations.shape, f32),
                pltpu.VMEM(cell_kind.shape, jnp.int32),
                pltpu.SemaphoreType.DMA((3,)),
                pltpu.VMEM((19, cx + 2, cy, nz), f32),
                pltpu.VMEM((cx, cy, nz), f32),
                pltpu.VMEM((5, cx, 1, nz), f32),
                pltpu.VMEM((5, cx, 1, nz), f32),
                pltpu.VMEM((5, cx, 1, nz), f32),
                pltpu.VMEM((5, cx, 1, nz), f32),
                pltpu.VMEM((5, cx + 2, 1, nz), f32),
                pltpu.VMEM((5, cx + 2, 1, nz), f32),
                pltpu.VMEM((1, 128), f32),
                pltpu.VMEM((ngx * ngy, 1, 128), f32),
                pltpu.VMEM((2, ngx, ngy, 128), f32),
                pltpu.VMEM((cx // TILE + 2, cy, nz), f32),
                pltpu.VMEM((cx // TILE + 2, 1, nz), f32),
                pltpu.VMEM((cx // TILE + 2, 1, nz), f32),
                pltpu.SemaphoreType.DMA((2, 8)),
                pltpu.SemaphoreType.DMA((2, 8)),
                pltpu.SemaphoreType.DMA((2,)),
            ],
            compiler_params=pltpu.CompilerParams(
                collective_id=0, has_side_effects=True, vmem_limit_bytes=48 * 2**20
            ),
        )(*[pltpu.with_memory_space_constraint(a, pltpu.HBM) for a in arrays])
        return pl.pallas_call(
            finish,
            out_shape=(
                jax.ShapeDtypeStruct(populations.shape, f32),
                jax.ShapeDtypeStruct((2, REGIONS), f32),
            ),
            in_specs=[vmem] * 7,
            out_specs=(hbm, vmem),
            scratch_shapes=[
                pltpu.VMEM(populations.shape, f32),
                pltpu.SemaphoreType.DMA((19,)),
            ],
            compiler_params=pltpu.CompilerParams(vmem_limit_bytes=16 * 2**20),
        )(*middle)

    in_specs = (P(None, "gx", "gy", None), P("gx", "gy", None), P("gx", "gy"))
    out_specs = (P(None, "gx", "gy", None), P())
    return jax.shard_map(body, mesh=mesh, in_specs=in_specs, out_specs=out_specs, check_vma=False)
```

```python
import functools

import jax
import jax.numpy as jnp
from jax import lax
from jax.experimental import pallas as pl
from jax.experimental.pallas import tpu as pltpu
from jax.sharding import PartitionSpec as P

REGIONS = 64
TILE = 4
VELOCITIES = (
    (0, 0, 0),
    (1, 0, 0),
    (-1, 0, 0),
    (0, 1, 0),
    (0, -1, 0),
    (0, 0, 1),
    (0, 0, -1),
    (1, 1, 0),
    (-1, -1, 0),
    (1, -1, 0),
    (-1, 1, 0),
    (1, 0, 1),
    (-1, 0, -1),
    (1, 0, -1),
    (-1, 0, 1),
    (0, 1, 1),
    (0, -1, -1),
    (0, 1, -1),
    (0, -1, 1),
)
NUMBER = {velocity: number for number, velocity in enumerate(VELOCITIES)}
WEIGHTS = (1.0 / 3.0,) + (1.0 / 18.0,) * 6 + (1.0 / 36.0,) * 12
OPPOSITE = (0, 2, 1, 4, 3, 6, 5, 8, 7, 10, 9, 12, 11, 14, 13, 16, 15, 18, 17)
RELAX_TIME = 0.8
INLET_SPEED = 0.05
RISING_X = (1, 7, 9, 11, 13)
FALLING_X = (2, 8, 10, 12, 14)
RISING_Y = (3, 7, 10, 15, 17)
FALLING_Y = (4, 8, 9, 16, 18)
SLOTS = RISING_X + FALLING_X + (0, 3, 4, 5, 6, 15, 16, 17, 18)
SLOT = {number: slot for slot, number in enumerate(SLOTS)}
MESH = pl.DeviceIdType.MESH


def inlet_value(number):
    comp_z = VELOCITIES[number][2]
    projected = comp_z * INLET_SPEED
    return WEIGHTS[number] * (
        1.0 + 3.0 * projected + 4.5 * projected * projected - 1.5 * INLET_SPEED * INLET_SPEED
    )


def signed_sum(terms):
    total = None
    for sign, value in terms:
        if total is None:
            total = value if sign > 0 else -value
        else:
            total = total + value if sign > 0 else total - value
    return total


def collide(current, kinds, outlet_density):
    density = functools.reduce(lambda a, b: a + b, current)
    inverse = 1.0 / density
    vel = [
        signed_sum([(v[d], current[n]) for n, v in enumerate(VELOCITIES) if v[d] != 0]) * inverse
        for d in range(3)
    ]
    base = 1.0 - 1.5 * (vel[0] * vel[0] + vel[1] * vel[1] + vel[2] * vel[2])
    wall = kinds == 1
    inlet = kinds == 2
    outlet = kinds == 3
    keep = jnp.where(outlet, 0.0, 1.0 - 1.0 / RELAX_TIME)
    scale = jnp.where(outlet, outlet_density, density * (1.0 / RELAX_TIME))
    scales = {w: scale * w for w in sorted(set(WEIGHTS))}
    post = [None] * 19
    for number in range(19):
        if number > OPPOSITE[number]:
            continue
        other = OPPOSITE[number]
        if number == 0:
            pairs = ((0, base),)
        else:
            projected = signed_sum([(c, vel[d]) for d, c in enumerate(VELOCITIES[number]) if c])
            even = base + 4.5 * projected * projected
            odd = 3.0 * projected
            pairs = ((number, even + odd), (other, even - odd))
        for n, unit in pairs:
            moved = keep * current[n] + scales[WEIGHTS[n]] * unit
            moved = jnp.where(inlet, inlet_value(n), moved)
            post[n] = jnp.where(wall, current[OPPOSITE[n]], moved)
    return density, post


def streamed(n, x, post, low, high, scales=None):
    vx, vy, vz = VELOCITIES[n]
    source = x + 1 - vx
    cy, nz = post.shape[2:]
    yrow = lax.broadcasted_iota(jnp.int32, (cy, nz), 0)
    value = post[SLOT[n], source]
    if scales:
        scale, scale_low, scale_high = [ref[(source + TILE - 1) // TILE] for ref in scales]
        value = value * scale
    if vy == 1:
        edge = low[RISING_Y.index(n), source]
        edge = edge * scale_low if scales else edge
        value = jnp.where(yrow == 0, edge, pltpu.roll(value, 1, 0))
    elif vy == -1:
        edge = high[FALLING_Y.index(n), source]
        edge = edge * scale_high if scales else edge
        value = jnp.where(yrow == cy - 1, edge, pltpu.roll(value, cy - 1, 0))
    if vz:
        value = pltpu.roll(value, vz % nz, 1)
    return value


def finish(post, low, high, means, mult, mult_low, mult_high, out_hbm, means_out, out_ref, sems):
    means_out[...] = means[...]
    copies = []
    for n in range(19):
        for x in range(out_ref.shape[1]):
            out_ref[n, x] = streamed(n, x, post, low, high, (mult, mult_low, mult_high))
        copies.append(pltpu.make_async_copy(out_ref.at[n], out_hbm.at[n], sems.at[n]))
        copies[-1].start()
    for copy in copies:
        copy.wait()


def kernel(
    ngx,
    ngy,
    cx,
    cy,
    region_hbm,
    pops_hbm,
    kind_hbm,
    post_b,
    low_b,
    high_b,
    means_ref,
    mult_b,
    mult_low_b,
    mult_high_b,
    region_ref,
    pops_ref,
    kind_ref,
    load_sems,
    post_a,
    density_ref,
    up_a,
    down_a,
    up_b,
    down_b,
    low_a,
    high_a,
    row_ref,
    table,
    spread,
    mult,
    mult_low,
    mult_high,
    send_sems,
    recv_sems,
    gather_sems,
):
    gx = lax.axis_index("gx")
    gy = lax.axis_index("gy")
    count = ngx * ngy
    me = gx * ngy + gy
    tx_n, ty_n = cx // TILE, cy // TILE
    nz = pops_ref.shape[3]
    lane = lax.broadcasted_iota(jnp.int32, (1, 128), 1)
    zlane = lax.broadcasted_iota(jnp.int32, (cy, nz), 1)
    yrow = lax.broadcasted_iota(jnp.int32, (cy, nz), 0)

    loads = [
        pltpu.make_async_copy(region_hbm, region_ref, load_sems.at[2]),
        pltpu.make_async_copy(pops_hbm, pops_ref, load_sems.at[0]),
        pltpu.make_async_copy(kind_hbm, kind_ref, load_sems.at[1]),
    ]
    for load in loads:
        load.start()
    barrier = pltpu.get_barrier_semaphore()

    def wrapped(value, size):
        return jnp.where(value >= size, value - size, value)

    def every_peer(visit):
        for turn in range(ngy):
            away = ngy - (turn + 1) // 2 if turn % 2 else turn // 2
            py = wrapped(ngy - 1 - gy + away, ngy)

            def one(ox, carry):
                visit({"gx": wrapped(gx + ox, ngx), "gy": py})
                return carry

            @pl.when(py != gy)
            def _():
                visit({"gx": gx, "gy": py})

            lax.fori_loop(1, ngx, one, 0, unroll=ngx <= 4)

    every_peer(
        lambda peer: pl.semaphore_signal(barrier, inc=1, device_id=peer, device_id_type=MESH)
    )

    def first(x, carry):
        current = [pops_ref[n, x] for n in range(19)]
        density, post = collide(current, kind_ref[x], 1.0)
        density_ref[x] = density
        for n in range(19):
            post_a[SLOT[n], x + 1] = post[n]
        for k in range(5):
            up_a[k, x] = post[RISING_Y[k]][cy - 1 :, :]
            down_a[k, x] = post[FALLING_Y[k]][:1, :]
        return carry

    for load in loads:
        load.wait()
    lax.fori_loop(0, cx, first, 0, unroll=2)

    sums = {}

    def put(key, value):
        sums[key] = value if key not in sums else sums[key] + value

    for tx in range(tx_n):
        for i in range(TILE):
            x = tx * TILE + i
            for vx in (-1, 0, 1):
                dx = vx if (vx == 1 and i == TILE - 1) or (vx == -1 and i == 0) else 0
                for vy in (-1, 0, 1):
                    flat = jnp.where(
                        zlane == nz - 1, post_a[SLOT[NUMBER[(vx, vy, 0)]], x + 1], 0.0
                    )
                    if (vx, vy, 1) in NUMBER:
                        rising = post_a[SLOT[NUMBER[(vx, vy, 1)]], x + 1]
                        falling = post_a[SLOT[NUMBER[(vx, vy, -1)]], x + 1]
                        flat = jnp.where(zlane == nz - 2, rising, flat)
                        flat = jnp.where(zlane == 0, falling, flat)
                    put((tx, dx, vy), flat)
            put((tx, "rho"), jnp.where(zlane == nz - 1, density_ref[x], 0.0))
    stage = jnp.zeros((cy, 128), jnp.float32)
    lane8 = lax.broadcasted_iota(jnp.int32, (cy, 128), 1)
    row8 = lax.broadcasted_iota(jnp.int32, (cy, 128), 0)
    block = 16 * ty_n
    for tx in range(tx_n):
        for dx in (-1, 0, 1):
            for vy in (-1, 0, 1):
                value = sums[(tx, dx, vy)]
                fixed = jnp.sum(jnp.where(zlane == nz - 1, 0.0, value), axis=1, keepdims=True)
                scaled = jnp.sum(jnp.where(zlane == nz - 1, value, 0.0), axis=1, keepdims=True)
                at = tx * block + (dx + 1) * 4 + vy + 1
                stage = jnp.where(lane8 == at, fixed, stage)
                stage = jnp.where(lane8 == 64 + at, scaled, stage)
        rho = jnp.sum(sums[(tx, "rho")], axis=1, keepdims=True)
        stage = jnp.where(lane8 == tx * block + 13, rho, stage)
    slot8 = lane8 & 3
    message = jnp.zeros((1, 128), jnp.float32)
    for ty in range(ty_n):
        first_row, last_row = ty * TILE, ty * TILE + TILE - 1
        inside = (row8 >= first_row) & (row8 <= last_row)
        crossing = ((slot8 == 2) & (row8 == last_row)) | ((slot8 == 0) & (row8 == first_row))
        cross = jnp.sum(jnp.where(crossing, stage, 0.0), axis=0, keepdims=True)
        stay = jnp.where(inside & jnp.logical_not(crossing), stage, 0.0)
        stay = jnp.broadcast_to(jnp.sum(stay, axis=0, keepdims=True), (8, 128))
        stay = (stay + pltpu.roll(stay, 1, 1) + pltpu.roll(stay, 127, 1))[:1]
        both = jnp.where((lane & 3) == 1, stay, cross)
        if ty:
            both = pltpu.roll(jnp.broadcast_to(both, (8, 128)), 16 * ty, 1)[:1]
        message = message + both
    for tx in range(tx_n):
        for ty in range(ty_n):
            region = region_ref[tx * TILE, ty * TILE].astype(jnp.float32)
            message = jnp.where(lane == 64 + tx * block + ty * 16 + 13, region, message)
    row_ref[...] = message
    table[me] = message

    pl.semaphore_wait(barrier, count - 1)

    every_peer(
        lambda peer: pltpu.make_async_remote_copy(
            src_ref=row_ref,
            dst_ref=table.at[me],
            send_sem=gather_sems.at[0],
            recv_sem=gather_sems.at[1],
            device_id=peer,
            device_id_type=MESH,
        ).start()
    )

    def exchange(step, post, up, down, low, high):
        def send(k, source, target, ox, oy):
            copy = pltpu.make_async_remote_copy(
                src_ref=source,
                dst_ref=target,
                send_sem=send_sems.at[step, k],
                recv_sem=recv_sems.at[step, k],
                device_id={"gx": lax.rem(gx + ox + ngx, ngx), "gy": lax.rem(gy + oy + ngy, ngy)},
                device_id_type=MESH,
            )
            copy.start()
            return copy

        return [
            send(0, up.at[RISING_Y.index(7), cx - 1], low.at[RISING_Y.index(7), 0], 1, 1),
            send(1, up.at[RISING_Y.index(10), 0], low.at[RISING_Y.index(10), cx + 1], -1, 1),
            send(2, down.at[FALLING_Y.index(9), cx - 1], high.at[FALLING_Y.index(9), 0], 1, -1),
            send(3, down.at[FALLING_Y.index(8), 0], high.at[FALLING_Y.index(8), cx + 1], -1, -1),
            send(4, up, low.at[:, pl.ds(1, cx)], 0, 1),
            send(5, down, high.at[:, pl.ds(1, cx)], 0, -1),
            send(6, post.at[pl.ds(0, 5), cx], post.at[pl.ds(0, 5), 0], 1, 0),
            send(7, post.at[pl.ds(5, 5), 1], post.at[pl.ds(5, 5), cx + 1], -1, 0),
        ]

    def rims(post, low, high):
        @pl.when(gx == 0)
        def _():
            post[0:5, 0] = jnp.zeros((5, cy, nz), jnp.float32)
            low[RISING_Y.index(7), 0] = jnp.zeros((1, nz), jnp.float32)
            high[FALLING_Y.index(9), 0] = jnp.zeros((1, nz), jnp.float32)

        @pl.when(gx == ngx - 1)
        def _():
            post[5:10, cx + 1] = jnp.zeros((5, cy, nz), jnp.float32)
            low[RISING_Y.index(10), cx + 1] = jnp.zeros((1, nz), jnp.float32)
            high[FALLING_Y.index(8), cx + 1] = jnp.zeros((1, nz), jnp.float32)

    copies = exchange(0, post_a, up_a, down_a, low_a, high_a)

    whole = pltpu.make_async_copy(
        table.at[pl.ds(0, count - 1)], table.at[pl.ds(0, count - 1)], gather_sems.at[1]
    )
    whole.wait()
    pltpu.make_async_copy(
        table.at[pl.ds(0, count - 1)], table.at[pl.ds(0, count - 1)], gather_sems.at[0]
    ).wait()

    tiles = tx_n * ty_n
    lanes = lax.broadcasted_iota(jnp.int32, (ngy, 128), 1)
    lanes_f = lanes.astype(jnp.float32)
    rows = [table[pl.ds(X * ngy, ngy), 0, :] for X in range(ngx)]
    onehot = {}
    total = jnp.zeros((ngy, 128), jnp.float32)
    cells = jnp.zeros((ngy, 128), jnp.float32)
    for X in range(ngx):
        for q in range(tiles):
            at = q * 16 + 13
            onehot[X, q] = rows[X][:, 64 + at : 65 + at] == lanes_f
            total = total + jnp.where(onehot[X, q], rows[X][:, at : at + 1], 0.0)
            cells = cells + jnp.where(onehot[X, q], 1.0 * TILE * TILE, 0.0)
    cells = jnp.sum(cells, axis=0, keepdims=True)
    cells = jnp.where(cells > 0.0, cells, 1.0)
    mean_1 = jnp.sum(total, axis=0, keepdims=True) / cells
    means_ref[0:1, :] = mean_1[:, :REGIONS]

    def by_region(mean, X):
        result = jnp.zeros((ngy, 128), jnp.float32)
        for q in range(tiles):
            m = jnp.sum(jnp.where(onehot[X, q], mean, 0.0), axis=1, keepdims=True)
            result = jnp.where((lanes >> 4) == q, m, result)
        return result

    by_tile = [by_region(mean_1, X) for X in range(ngx)]
    for X in range(ngx):
        spread[0, X] = by_tile[X]

    zrow = lax.broadcasted_iota(jnp.int32, (1, nz), 1)

    def scale_outlets(step, mult, mult_low, mult_high):
        around = {}
        for ox in (-1, 0, 1):
            for oy in (-1, 0, 1):
                sx = jnp.clip(gx + ox, 0, ngx - 1)
                sy = lax.rem(gy + oy + ngy, ngy)
                around[ox, oy] = spread[step, sx, pl.ds(sy, 1), :]

        def tile_mean(tx, ty):
            ox = -1 if tx < 0 else 1 if tx >= tx_n else 0
            oy = -1 if ty < 0 else 1 if ty >= ty_n else 0
            at = ((tx - ox * tx_n) * ty_n + ty - oy * ty_n) * 16
            return around[ox, oy][:, at : at + 1]

        for k in range(tx_n + 2):
            column = tile_mean(k - 1, 0)
            for ty in range(1, ty_n):
                column = jnp.where(yrow >= ty * TILE, tile_mean(k - 1, ty), column)
            mult[k] = jnp.where(zlane == nz - 1, column, 1.0)
            mult_low[k] = jnp.where(zrow == nz - 1, tile_mean(k - 1, -1), 1.0)
            mult_high[k] = jnp.where(zrow == nz - 1, tile_mean(k - 1, ty_n), 1.0)

    scale_outlets(0, mult, mult_low, mult_high)

    for copy in copies:
        copy.wait()
    rims(post_a, low_a, high_a)

    def second(x, carry):
        current = [
            streamed(n, x, post_a, low_a, high_a, (mult, mult_low, mult_high)) for n in range(19)
        ]
        _, post = collide(current, kind_ref[x], 1.0)
        for n in range(19):
            post_b[SLOT[n], x + 1] = post[n]
        for k in range(5):
            up_b[k, x] = post[RISING_Y[k]][cy - 1 :, :]
            down_b[k, x] = post[FALLING_Y[k]][:1, :]
        return carry

    lax.fori_loop(0, cx, second, 0, unroll=cx)

    copies = exchange(1, post_b, up_b, down_b, low_b, high_b)

    tile_x, tile_y = (lanes >> 4) // ty_n, (lanes >> 4) % ty_n
    step_x, step_y = ((lanes >> 2) & 3) - 1, (lanes & 3) - 1
    real = (lanes < 16 * tiles) & (step_x < 2) & (step_y < 2)
    to_x, to_y = tile_x + step_x, tile_y + step_y
    off_x = jnp.where(to_x < 0, -1, jnp.where(to_x >= tx_n, 1, 0))
    off_y = jnp.where(to_y < 0, -1, jnp.where(to_y >= ty_n, 1, 0))
    goal = (to_x - off_x * tx_n) * ty_n + (to_y - off_y * ty_n)
    shifted = []
    for X in range(ngx):
        value = jnp.where(real, rows[X] + by_tile[X] * pltpu.roll(rows[X], 64, 1), 0.0)
        moved = jnp.where(off_y == 0, value, 0.0)
        moved = moved + pltpu.roll(jnp.where(off_y == 1, value, 0.0), 1, 0)
        moved = moved + pltpu.roll(jnp.where(off_y == -1, value, 0.0), ngy - 1, 0)
        shifted.append(moved)
    total = jnp.zeros((ngy, 128), jnp.float32)
    for X in range(ngx):
        landed = jnp.where(off_x == 0, shifted[X], 0.0)
        if X > 0:
            landed = landed + jnp.where(off_x == 1, shifted[X - 1], 0.0)
        if X < ngx - 1:
            landed = landed + jnp.where(off_x == -1, shifted[X + 1], 0.0)
        for q in range(tiles):
            s = jnp.sum(jnp.where(goal == q, landed, 0.0), axis=1, keepdims=True)
            total = total + jnp.where(onehot[X, q], s, 0.0)
    mean_2 = jnp.sum(total, axis=0, keepdims=True) / cells
    means_ref[1:2, :] = mean_2[:, :REGIONS]

    for X in range(ngx):
        spread[1, X] = by_region(mean_2, X)
    scale_outlets(1, mult_b, mult_low_b, mult_high_b)

    for copy in copies:
        copy.wait()
    rims(post_b, low_b, high_b)


def solution(mesh):
    ngx, ngy = mesh.shape["gx"], mesh.shape["gy"]

    def body(populations, cell_kind, outlet_region):
        _, cx, cy, nz = populations.shape
        f32 = jnp.float32
        arrays = (outlet_region, populations, cell_kind)
        vmem = pl.BlockSpec(memory_space=pltpu.VMEM)
        hbm = pl.BlockSpec(memory_space=pltpu.HBM)
        middle = pl.pallas_call(
            functools.partial(kernel, ngx, ngy, cx, cy),
            out_shape=(
                pltpu.VMEM((19, cx + 2, cy, nz), f32),
                pltpu.VMEM((5, cx + 2, 1, nz), f32),
                pltpu.VMEM((5, cx + 2, 1, nz), f32),
                pltpu.VMEM((2, REGIONS), f32),
                pltpu.VMEM((cx // TILE + 2, cy, nz), f32),
                pltpu.VMEM((cx // TILE + 2, 1, nz), f32),
                pltpu.VMEM((cx // TILE + 2, 1, nz), f32),
            ),
            in_specs=[hbm, hbm, hbm],
            out_specs=(vmem,) * 7,
            scratch_shapes=[
                pltpu.SMEM(outlet_region.shape, jnp.int32),
                pltpu.VMEM(populations.shape, f32),
                pltpu.VMEM(cell_kind.shape, jnp.int32),
                pltpu.SemaphoreType.DMA((3,)),
                pltpu.VMEM((19, cx + 2, cy, nz), f32),
                pltpu.VMEM((cx, cy, nz), f32),
                pltpu.VMEM((5, cx, 1, nz), f32),
                pltpu.VMEM((5, cx, 1, nz), f32),
                pltpu.VMEM((5, cx, 1, nz), f32),
                pltpu.VMEM((5, cx, 1, nz), f32),
                pltpu.VMEM((5, cx + 2, 1, nz), f32),
                pltpu.VMEM((5, cx + 2, 1, nz), f32),
                pltpu.VMEM((1, 128), f32),
                pltpu.VMEM((ngx * ngy, 1, 128), f32),
                pltpu.VMEM((2, ngx, ngy, 128), f32),
                pltpu.VMEM((cx // TILE + 2, cy, nz), f32),
                pltpu.VMEM((cx // TILE + 2, 1, nz), f32),
                pltpu.VMEM((cx // TILE + 2, 1, nz), f32),
                pltpu.SemaphoreType.DMA((2, 8)),
                pltpu.SemaphoreType.DMA((2, 8)),
                pltpu.SemaphoreType.DMA((2,)),
            ],
            compiler_params=pltpu.CompilerParams(
                collective_id=0, has_side_effects=True, vmem_limit_bytes=48 * 2**20
            ),
        )(*[pltpu.with_memory_space_constraint(a, pltpu.HBM) for a in arrays])
        return pl.pallas_call(
            finish,
            out_shape=(
                jax.ShapeDtypeStruct(populations.shape, f32),
                jax.ShapeDtypeStruct((2, REGIONS), f32),
            ),
            in_specs=[vmem] * 7,
            out_specs=(hbm, vmem),
            scratch_shapes=[
                pltpu.VMEM(populations.shape, f32),
                pltpu.SemaphoreType.DMA((19,)),
            ],
            compiler_params=pltpu.CompilerParams(vmem_limit_bytes=16 * 2**20),
        )(*middle)

    in_specs = (P(None, "gx", "gy", None), P("gx", "gy", None), P("gx", "gy"))
    out_specs = (P(None, "gx", "gy", None), P())
    return jax.shard_map(body, mesh=mesh, in_specs=in_specs, out_specs=out_specs, check_vma=False)
```
